32 devices in a mesh: pipe: 2 (over core), seq: 8 (over z, x), tp: 2 (over y).
Axes of the slice: x: 2, y: 2, z: 4, core: 2. Of those that a mesh axis runs over, the one named last changes fastest.
Arguments:
- hidden_in: bfloat16 [1, 4096, 2560], P(None, ('seq', 'tp')), may hold values from -6 to 6
- doc_ids: int32 [1, 4096], P(None, 'seq'), may hold values from 0 to 1, never falling along the last dimension, each value on 1 to 3072 neighbouring positions
- norm_gain: float32 [2, 2560], P('pipe'), may hold values from 0.1 to 1.9
- in_zx: bfloat16 [2, 2560, 2, 5120], P('pipe', None, None, 'tp'), may hold values from -0.125 to 0.125
- in_bc: bfloat16 [2, 2560, 256], P('pipe'), may hold values from -0.125 to 0.125
- in_dt: bfloat16 [2, 2560, 80], P('pipe', None, 'tp'), may hold values from -0.125 to 0.125
- conv_x: float32 [2, 4, 5120], P('pipe', None, 'tp'), may hold values from -3 to 3
- conv_bc: float32 [2, 4, 256], P('pipe'), may hold values from -3 to 3
- bias_x: float32 [2, 5120], P('pipe', 'tp'), may hold values from -3 to 3
- bias_bc: float32 [2, 256], P('pipe'), may hold values from -3 to 3
- dt_bias: float32 [2, 80], P('pipe', 'tp'), may hold values from -2 to 1
- a_log: float32 [2, 80], P('pipe', 'tp'), may hold values from -12 to 0, as said below
- d_skip: float32 [2, 80], P('pipe', 'tp'), may hold values from 0.5 to 1.5
- gated_gain: float32 [2, 5120], P('pipe', 'tp'), may hold values from 0.1 to 1.9
- out_w: bfloat16 [2, 5120, 2560], P('pipe', 'tp'), may hold values from -0.078125 to 0.078125
Outputs:
- section_out: bfloat16 [2, 1, 4096, 2560], P('pipe', None, ('seq', 'tp'))
The draws below stay inside these ranges and needn't reach their ends.
Inputs may be any that keep to these rules, and one draw needn't show every extreme that they name: `doc_ids`: in each row the document numbers start at 0, never fall, and rise by one where a new document begins; every document spans 1 to 3072 positions. `a_log`: logarithms of rates between 0.5 / 4096 and 1.
All inputs are finite; a program needn't handle non-finite values.
Results may differ from the reference program's by a relative error of at most 0.02.
Values may be sent and summed in bfloat16 or wider, within the bound.
A program may use at most 192 MiB of HBM per device.

```python
import math
import jax
import jax.numpy as jnp
import numpy as np
from jax import lax

D = 2560
E = 5120
H = 80
HEADDIM = 64
NS = 128
KW = 4
BLOCK = 256
MB = 1
SEQLEN = 4096
LAYERS = 2


def draw_a_log(key, part):
    uniform_draw = jax.random.uniform(key, (LAYERS, H), jnp.float32)
    lowest = math.log(0.5 / SEQLEN)
    return (lowest * (1.0 - uniform_draw)).astype(jnp.float32)


def block_scale(stream_key, extent, pieces, least, high):
    def one(axis_at, blocks):
        steps = jax.random.uniform(jax.random.fold_in(jax.random.fold_in(stream_key, 6), axis_at), (blocks,), jnp.float32, least / len(pieces), high / len(pieces))
        return jnp.repeat(jnp.exp(steps), extent[axis_at] // blocks).reshape((-1,) + (1,) * (len(extent) - axis_at - 1))

    loudness = one(*pieces[0])
    for cut in pieces[1:]:
        loudness = loudness * one(*cut)
    return loudness


def profile(count, total, bound, slope):
    portions = [(1 << 20) // math.isqrt(standing ** slope) + 1 for standing in range(2, count + 1)]
    spare, given = total - bound - (count - 1), [1] * (count - 1)
    while spare > 0:
        movable = [i for i in range(count - 1) if given[i] < bound]
        whole, remaining = sum([portions[i] for i in movable]), spare
        for i in movable:
            addition = min(bound - given[i], max(1, remaining * portions[i] // whole), spare)
            given[i] = given[i] + addition
            spare = spare - addition
    return np.array([bound] + given)


def uneven(own_key, number_of, total, limit, lean):
    if number_of == 2:
        one = jax.random.randint(own_key, (), max(1, total - limit), min(limit, total - 1) + 1)
        return jnp.stack([one, total - one])
    tallies = jnp.asarray(profile(number_of, total, limit, lean), jnp.int32)
    couples = (number_of - 1) // 2
    source_of, taker = tallies[1:1 + 2 * couples:2], tallies[2:2 + 2 * couples:2]
    slack = jnp.minimum(source_of - 1, limit - taker)
    passed = jax.random.randint(jax.random.fold_in(own_key, 1), (couples,), 0, 1 << 20) % (slack + 1)
    tallies = tallies.at[1:1 + 2 * couples:2].set(source_of - passed).at[2:2 + 2 * couples:2].set(taker + passed)
    return tallies[jax.random.permutation(jax.random.fold_in(own_key, 2), number_of)]


def gaussian(key, extent, scale, bound, shards=(), dtype=jnp.bfloat16):
    entries = scale * jax.random.normal(key, extent, jnp.float32)
    if shards:
        entries = entries * block_scale(key, extent, shards, -0.22, 0.18)
    return jnp.clip(entries, -bound, bound).astype(dtype)


def setup_inputs(seed: int = 0) -> dict:
    arg_keys = jax.random.split(jax.random.key(seed), 16)
    hidden_in = gaussian(arg_keys[0], (MB, SEQLEN, D), 1.0, 6.0, ((1, 16),))
    doc_ids = jax.vmap(lambda own: jnp.searchsorted(jnp.cumsum(uneven(own, 2, SEQLEN, 3 * SEQLEN // 4, 0)), jnp.arange(SEQLEN), side="right"))(jax.random.split(arg_keys[1], MB)).reshape((MB, SEQLEN)).astype(jnp.int32)
    norm_gain = jnp.clip(1.0 + 0.18 * jax.random.normal(arg_keys[2], (LAYERS, D), jnp.float32), 0.1, 1.9)
    in_zx = gaussian(arg_keys[3], (LAYERS, D, 2, E), D ** -0.5, 0.125, ((0, 2), (3, 2)))
    in_bc = gaussian(arg_keys[4], (LAYERS, D, 2 * NS), D ** -0.5, 0.125, ((0, 2),))
    in_dt = gaussian(arg_keys[5], (LAYERS, D, H), D ** -0.5, 0.125, ((0, 2), (2, 2)))
    conv_x = gaussian(arg_keys[6], (LAYERS, KW, E), KW ** -0.5, 3.0, ((0, 2), (2, 2)), jnp.float32)
    conv_bc = gaussian(arg_keys[7], (LAYERS, KW, 2 * NS), KW ** -0.5, 3.0, ((0, 2),), jnp.float32)
    bias_x = gaussian(arg_keys[8], (LAYERS, E), 0.5, 3.0, ((0, 2), (1, 2)), jnp.float32)
    bias_bc = gaussian(arg_keys[9], (LAYERS, 2 * NS), 0.5, 3.0, ((0, 2),), jnp.float32)
    dt_bias = jnp.clip(-2.0 + 3.0 * jax.random.uniform(arg_keys[10], (LAYERS, H), jnp.float32) ** block_scale(arg_keys[10], (LAYERS, H), ((0, 2), (1, 2)), -0.2, 0.2), -2.0, 1.0)
    a_log = draw_a_log(jax.random.fold_in(arg_keys[15], 71), 0)
    d_skip = jnp.clip(0.5 + 1.0 * jax.random.uniform(arg_keys[12], (LAYERS, H), jnp.float32) ** block_scale(arg_keys[12], (LAYERS, H), ((0, 2), (1, 2)), -0.2, 0.2), 0.5, 1.5)
    gated_gain = jnp.clip(1.0 + 0.18 * jax.random.normal(arg_keys[13], (LAYERS, E), jnp.float32), 0.1, 1.9)
    out_w = gaussian(arg_keys[14], (LAYERS, E, D), E ** -0.5, 0.078125, ((0, 2), (1, 2)))
    return dict(hidden_in=hidden_in, doc_ids=doc_ids, norm_gain=norm_gain, in_zx=in_zx, in_bc=in_bc, in_dt=in_dt, conv_x=conv_x, conv_bc=conv_bc, bias_x=bias_x, bias_bc=bias_bc, dt_bias=dt_bias, a_log=a_log, d_skip=d_skip, gated_gain=gated_gain, out_w=out_w)


epsilon = 1e-05
highest = lax.Precision.HIGHEST

def conv_mix(row_block, edge_rows, row_ids, edge_ids, weight, shift_bias):
    padded = jnp.concatenate([edge_rows, row_block], 0)
    padded_ids = jnp.concatenate([edge_ids, row_ids], 0)
    row_count = row_block.shape[0]
    running = jnp.zeros_like(row_block) + shift_bias[None, :]
    for offset in range(weight.shape[0]):
        keep_mask = (padded_ids[offset:offset + row_count] == row_ids).astype(jnp.float32)
        running = running + keep_mask[:, None] * weight[offset][None, :] * padded[offset:offset + row_count]
    return jax.nn.silu(running)

def block_step(state_in, inputs, decay_rates):
    x_block, step_sizes, b_block, c_block, seg_block, prev_id = inputs
    log_decay = jnp.cumsum(step_sizes * decay_rates[:, None], axis=1)
    block_length = seg_block.shape[0]
    causal_mask = jnp.arange(block_length)[:, None] >= jnp.arange(block_length)[None, :]
    same_doc = causal_mask & (seg_block[:, None] == seg_block[None, :])
    spread = log_decay[:, :, None] - log_decay[:, None, :]
    mixing = jnp.where(same_doc[None], jnp.exp(jnp.where(same_doc[None], spread, 0.0)), 0.0)
    gram_matrix = jnp.dot(c_block, b_block.T, precision=highest)
    weights = mixing * gram_matrix[None] * step_sizes[:, None, :]
    outputs = jnp.einsum('hps,hts->hpt', x_block, weights, precision=highest)
    carried = (seg_block == prev_id).astype(jnp.float32)
    outputs = outputs + jnp.exp(log_decay)[:, None, :] * carried[None, None, :] * jnp.einsum('hpn,tn->hpt', state_in, c_block, precision=highest)
    end_weight = jnp.exp(log_decay[:, -1:] - log_decay) * (seg_block == seg_block[-1]).astype(jnp.float32)[None, :] * step_sizes
    fresh_state = jnp.einsum('hps,sn->hpn', x_block * end_weight[:, None, :], b_block, precision=highest)
    keep_all = jnp.exp(log_decay[:, -1]) * (seg_block[-1] == prev_id).astype(jnp.float32)
    return (keep_all[:, None, None] * state_in + fresh_state, outputs)

def mamba_layer(hidden, row_ids, norm_scale, weight_zx, weight_bc, weight_dt, kernel_x, kernel_bc, offset_x, offset_bc, dt_shift, log_rate, skip_scale, gate_scale, weight_out):
    hidden_f = hidden.astype(jnp.float32)
    normed = (hidden_f * lax.rsqrt(lax.optimization_barrier(jnp.mean(hidden_f * hidden_f, axis=1, keepdims=True)) + epsilon) * norm_scale[None, :]).astype(jnp.bfloat16)
    gate_in = jnp.dot(normed, weight_zx[:, 0, :], preferred_element_type=jnp.float32)
    x_raw = jnp.dot(normed, weight_zx[:, 1, :], preferred_element_type=jnp.float32)
    bc_raw = jnp.dot(normed, weight_bc, preferred_element_type=jnp.float32)
    dt_raw = jnp.dot(normed, weight_dt, preferred_element_type=jnp.float32)
    pre_conv = jnp.concatenate([x_raw, bc_raw], 1)
    kernel = jnp.concatenate([kernel_x, kernel_bc], 1)
    kernel_bias = jnp.concatenate([offset_x, offset_bc], 0)
    edge_rows = jnp.zeros((KW - 1, E + 2 * NS), jnp.float32)
    edge_ids = jnp.full((KW - 1,), -1, jnp.int32)
    conv_out = conv_mix(pre_conv, edge_rows, row_ids, edge_ids, kernel, kernel_bias)
    x_heads = conv_out[:, :E].T.reshape(H, HEADDIM, SEQLEN)
    b_conv = conv_out[:, E:E + NS]
    c_conv = conv_out[:, E + NS:]
    step_sizes = jax.nn.softplus(dt_raw + dt_shift[None, :]).T
    decay_rates = -jnp.exp(log_rate)
    blocks = SEQLEN // BLOCK
    prev_ids = jnp.concatenate([row_ids[:1], row_ids[BLOCK - 1:SEQLEN - 1:BLOCK]], 0)
    stacked = (x_heads.reshape(H, HEADDIM, blocks, BLOCK).transpose(2, 0, 1, 3), step_sizes.reshape(H, blocks, BLOCK).transpose(1, 0, 2), b_conv.reshape(blocks, BLOCK, NS), c_conv.reshape(blocks, BLOCK, NS), row_ids.reshape(blocks, BLOCK), prev_ids)

    def scan_body(state_in, inputs):
        return block_step(state_in, inputs, decay_rates)
    final_state, outputs = lax.scan(scan_body, jnp.zeros((H, HEADDIM, NS), jnp.float32), stacked)
    outputs = outputs.transpose(1, 2, 0, 3).reshape(H, HEADDIM, SEQLEN)
    outputs = outputs + skip_scale[:, None, None] * x_heads
    gated_rows = outputs.reshape(E, SEQLEN).T * jax.nn.silu(gate_in)
    branch_in = (gated_rows * lax.rsqrt(lax.optimization_barrier(jnp.mean(gated_rows * gated_rows, axis=1, keepdims=True)) + epsilon) * gate_scale[None, :]).astype(jnp.bfloat16)
    return (hidden_f + jnp.dot(branch_in, weight_out, preferred_element_type=jnp.float32)).astype(jnp.bfloat16)

def reference(hidden_in, doc_ids, norm_gain, in_zx, in_bc, in_dt, conv_x, conv_bc, bias_x, bias_bc, dt_bias, a_log, d_skip, gated_gain, out_w):
    per_layer = [[None] * MB for layer_index in range(LAYERS)]
    for micro_index in range(MB):
        hidden = hidden_in[micro_index]
        row_ids = doc_ids[micro_index]
        for layer_index in range(LAYERS):
            hidden = mamba_layer(hidden, row_ids, norm_gain[layer_index], in_zx[layer_index], in_bc[layer_index], in_dt[layer_index], conv_x[layer_index], conv_bc[layer_index], bias_x[layer_index], bias_bc[layer_index], dt_bias[layer_index], a_log[layer_index], d_skip[layer_index], gated_gain[layer_index], out_w[layer_index])
            per_layer[layer_index][micro_index] = hidden
    return jnp.stack([jnp.stack(micro_list) for micro_list in per_layer])
```

```python
import functools

import jax
import jax.numpy as jnp
from jax import lax
from jax.experimental import pallas as pl
from jax.experimental.pallas import tpu as pltpu
from jax.sharding import PartitionSpec as P

epsilon = 1e-05
LOG2E = 1.4426950408889634
HALO = 16
CHUNK = 128
LANES = 128
MESH = pl.DeviceIdType.MESH
f32 = jnp.float32
bf16 = jnp.bfloat16


def live_shift(block, axis, distance, live, wrap=False):
    size = lax.axis_size(axis)
    route = []
    for i in range(size):
        j = i + distance
        if wrap or j < size:
            route.append((live * size + i, live * size + j % size))
    return lax.ppermute(block, ("pipe", axis), route)


def gathered_rows(rows, axis, live):
    size = lax.axis_size(axis)
    place = lax.axis_index(axis)
    count = rows.shape[0]
    whole = jnp.zeros((size * count,) + rows.shape[1:], rows.dtype)
    whole = lax.dynamic_update_slice_in_dim(whole, rows, place * count, 0)
    for step in range(1, size):
        other = live_shift(rows, axis, step, live, True)
        source = lax.rem(place - step + size, size)
        whole = lax.dynamic_update_slice_in_dim(whole, other, source * count, 0)
    return whole


def scattered_sum(rows, squares, axis, live):
    size = lax.axis_size(axis)
    place = lax.axis_index(axis)
    count = rows.shape[0] // size
    total = lax.dynamic_slice_in_dim(rows, place * count, count, 0)
    square = lax.dynamic_slice_in_dim(squares, place * count, count, 0)
    for step in range(1, size):
        target = lax.rem(place + step, size)
        piece = lax.dynamic_slice_in_dim(rows, target * count, count, 0).astype(bf16)
        term = lax.dynamic_slice_in_dim(squares, target * count, count, 0)
        total = total + live_shift(piece, axis, step, live, True).astype(f32)
        square = square + live_shift(term, axis, step, live, True)
    return total, square


def silu(value):
    half = 0.5 * value
    return half + half * jnp.tanh(half)


def split_pair(value):
    high = value.astype(bf16)
    low = (value - high.astype(f32)).astype(bf16)
    return jnp.concatenate([high, low], 1)


def mixer_kernel(
    live,
    zx_ref,
    bcdt_ref,
    idc_ref,
    idr_ref,
    wx_ref,
    wbc_ref,
    hv_ref,
    g_ref,
    ss_ref,
    mask_s,
    l_s,
    m_s,
    lg_s,
    ew_s,
    cw_s,
    keep_s,
    b_s,
    c_s,
    gm_s,
    xc_s,
    fresh_s,
    y_s,
    send_s,
    recv_s,
    ksend_s,
    krecv_s,
    back_s,
    inc_s,
    send_sem,
    recv_sem,
    ksend_sem,
    krecv_sem,
    bsend_sem,
    brecv_sem,
):
    size = lax.axis_size("seq")
    me = lax.axis_index("seq")
    rows = g_ref.shape[0]
    width = g_ref.shape[1]
    chunks = rows // CHUNK
    tiles = width // LANES
    states = b_s.shape[1]
    slab = states // size
    heads_pad = hv_ref.shape[1]
    head_width = LANES // 2

    def lane_iota(shape):
        return lax.broadcasted_iota(jnp.int32, shape, 1)

    def row_iota(shape):
        return lax.broadcasted_iota(jnp.int32, shape, 0)

    def selector(tile, count, dtype):
        shape = (count, LANES)
        hit = lax.rem(row_iota(shape), heads_pad) == tile * 2 + lane_iota(shape) // head_width
        return hit.astype(f32).astype(dtype)

    def hop(source, target_ref, distance, send, recv):
        return pltpu.make_async_remote_copy(
            src_ref=source,
            dst_ref=target_ref,
            send_sem=send.at[distance - 1],
            recv_sem=recv.at[distance - 1],
            device_id={"seq": lax.rem(me + distance, size)},
            device_id_type=MESH,
        )

    @pl.when(lax.axis_index("pipe") == live)
    def _():
        barrier = pltpu.get_barrier_semaphore()
        for distance in range(1, size):
            pl.semaphore_signal(
                barrier,
                inc=1,
                device_id={"seq": lax.rem(me + distance, size)},
                device_id_type=MESH,
            )

        square_shape = (CHUNK, CHUNK)
        lower = row_iota(square_shape) >= lane_iota(square_shape)
        lower_f = lower.astype(f32)

        @pl.loop(0, chunks)
        def _(k):
            base = pl.multiple_of(k * CHUNK, CHUNK)
            here = pl.ds(base, CHUNK)
            ids_ext = idc_ref[pl.ds(base, CHUNK + HALO), :]
            seg = ids_ext[HALO:]
            prev = ids_ext[HALO - 1 : HALO]
            last = ids_ext[HALO + CHUNK - 1 :]
            for d in range(1, 4):
                same = pltpu.roll(ids_ext, d, 0)[HALO:] == seg
                mask_s[d - 1, here, :] = same.astype(f32)
            raw = bcdt_ref[pl.ds(base + HALO, CHUNK), 2 * states :] + hv_ref[0:1, :]
            step = jnp.maximum(raw, 0.0) + jnp.log1p(jnp.exp(-jnp.abs(raw)))
            level = jnp.dot(
                lower_f,
                step * hv_ref[1:2, :],
                precision=lax.Precision.HIGHEST,
                preferred_element_type=f32,
            )
            l_s[here, :] = level
            step_log = jnp.log(step) * LOG2E
            m_s[k] = (level - step_log).T
            lg_s[k] = step_log.T
            end = level[CHUNK - 1 :]
            ew_s[here, :] = split_pair(
                jnp.exp2(end - level) * step * (seg == last).astype(f32)
            )
            cw_s[here, :] = split_pair(jnp.exp2(level) * (seg == prev).astype(f32))
            keep_s[k] = jnp.broadcast_to(jnp.exp2(end) * (last == prev).astype(f32), (8, heads_pad))
            for half in range(2):
                cols = pl.ds(half * states, states)
                wide = bcdt_ref[pl.ds(base, CHUNK + HALO), cols]
                total = wbc_ref[4:5, cols] + wbc_ref[3:4, cols] * wide[HALO:]
                for d in range(1, 4):
                    total += (
                        mask_s[d - 1, here, :]
                        * wbc_ref[3 - d : 4 - d, cols]
                        * pltpu.roll(wide, d, 0)[HALO:]
                    )
                place = b_s if half == 0 else c_s
                place[here, :] = silu(total).astype(bf16)
            gram = lax.dot_general(
                c_s[here, :], b_s[here, :], (((1,), (1,)), ((), ())), preferred_element_type=f32
            )
            same_doc = seg == idr_ref[0:1, pl.ds(base, CHUNK)]
            gm_s[k] = jnp.where(lower & same_doc, gram, 0.0)

        @pl.loop(0, tiles)
        def _(tile):
            lanes = pl.ds(pl.multiple_of(tile * LANES, LANES), LANES)
            x_lanes = pl.ds(pl.multiple_of(width + tile * LANES, LANES), LANES)
            pick = selector(tile, 2 * heads_pad, bf16)
            pick_f = selector(tile, heads_pad, f32)
            state = jnp.zeros((states, LANES), f32)
            keep_all = jnp.ones((8, LANES), f32)
            for k in range(chunks):
                here = pl.ds(k * CHUNK, CHUNK)
                wide = zx_ref[pl.ds(k * CHUNK, CHUNK + HALO), x_lanes].astype(f32)
                total = wx_ref[4:5, lanes] + wx_ref[3:4, lanes] * wide[HALO:]
                for d in range(1, 4):
                    total += (
                        mask_s[d - 1, here, :]
                        * wx_ref[3 - d : 4 - d, lanes]
                        * pltpu.roll(wide, d, 0)[HALO:]
                    )
                conv = silu(total)
                xc_s[here, lanes] = conv.astype(bf16)
                weight = jnp.dot(ew_s[here, :], pick, preferred_element_type=f32)
                fresh = lax.dot_general(
                    b_s[here, :],
                    (conv * weight).astype(bf16),
                    (((0,), (0,)), ((), ())),
                    preferred_element_type=f32,
                )
                fresh_s[k, :, lanes] = fresh
                keep = jnp.dot(
                    keep_s[k], pick_f, precision=lax.Precision.HIGHEST, preferred_element_type=f32
                )
                state = state * keep[0:1] + fresh
                keep_all = keep_all * keep
            for part in range(size):
                send_s[part, :, lanes] = state[part * slab : (part + 1) * slab].astype(bf16)
            ksend_s[:, lanes] = keep_all[0:1]

        pl.semaphore_wait(barrier, size - 1)
        for distance in range(1, size):
            target = lax.rem(me + distance, size)
            hop(send_s.at[target], recv_s.at[me], distance, send_sem, recv_sem).start()
            hop(ksend_s, krecv_s.at[me], distance, ksend_sem, krecv_sem).start()
        recv_s[me] = send_s[me]
        krecv_s[me] = ksend_s[...]

        @pl.loop(0, tiles)
        def _(tile):
            lanes = pl.ds(pl.multiple_of(tile * LANES, LANES), LANES)
            first_half = lane_iota((CHUNK, LANES)) < head_width
            for k in range(chunks):
                here = pl.ds(k * CHUNK, CHUNK)
                level = l_s[here, :]
                gram = gm_s[k]
                mixes = []
                for j in range(2):
                    head = tile * 2 + j
                    column = pltpu.roll(level, heads_pad - head, 1)[:, 0:1]
                    shift = column - m_s[k, pl.ds(head, 1), :]
                    shift = jnp.minimum(shift, lg_s[k, pl.ds(head, 1), :])
                    mixes.append((jnp.exp2(shift) * gram).astype(bf16))
                conv = xc_s[here, lanes]
                zero = jnp.zeros_like(conv)
                both = jnp.concatenate(
                    [jnp.where(first_half, conv, zero), jnp.where(first_half, zero, conv)], 0
                )
                out = jnp.dot(jnp.concatenate(mixes, 1), both, preferred_element_type=f32)
                y_s[here, lanes] = out + wx_ref[5:6, lanes] * conv.astype(f32)

        for distance in range(1, size):
            source = lax.rem(me - distance + size, size)
            hop(send_s.at[me], recv_s.at[source], distance, send_sem, recv_sem).wait_recv()
            hop(ksend_s, krecv_s.at[source], distance, ksend_sem, krecv_sem).wait_recv()
        run = jnp.zeros((slab, width), f32)
        for part in range(size):
            back_s[part] = run.astype(bf16)
            if part < size - 1:
                run = run * krecv_s[part] + recv_s[part].astype(f32)
        for distance in range(1, size):
            target = lax.rem(me + distance, size)
            hop(back_s.at[target], inc_s.at[me], distance, bsend_sem, brecv_sem).start()
        inc_s[me] = back_s[me]
        for distance in range(1, size):
            source = lax.rem(me - distance + size, size)
            hop(back_s.at[me], inc_s.at[source], distance, bsend_sem, brecv_sem).wait_recv()

        ss_ref[...] = jnp.zeros_like(ss_ref)

        @pl.loop(0, tiles)
        def _(tile):
            lanes = pl.ds(pl.multiple_of(tile * LANES, LANES), LANES)
            pick = selector(tile, 2 * heads_pad, bf16)
            pick_f = selector(tile, heads_pad, f32)
            state = jnp.concatenate(
                [inc_s[part, :, lanes].astype(f32) for part in range(size)], 0
            )
            for k in range(chunks):
                here = pl.ds(k * CHUNK, CHUNK)
                weight = jnp.dot(cw_s[here, :], pick, preferred_element_type=f32)
                carried = jnp.dot(c_s[here, :], state.astype(bf16), preferred_element_type=f32)
                out = y_s[here, lanes] + weight * carried
                gate = zx_ref[pl.ds(k * CHUNK + HALO, CHUNK), lanes].astype(f32)
                out = out * silu(gate)
                ss_ref[here, :] += out * out
                g_ref[here, lanes] = (out * wx_ref[6:7, lanes]).astype(bf16)
                if k < chunks - 1:
                    keep = jnp.dot(
                        keep_s[k],
                        pick_f,
                        precision=lax.Precision.HIGHEST,
                        preferred_element_type=f32,
                    )
                    state = state * keep[0:1] + fresh_s[k, :, lanes]

        for distance in range(1, size):
            target = lax.rem(me + distance, size)
            hop(send_s.at[target], recv_s.at[me], distance, send_sem, recv_sem).wait_send()
            hop(ksend_s, krecv_s.at[me], distance, ksend_sem, krecv_sem).wait_send()
            hop(back_s.at[target], inc_s.at[me], distance, bsend_sem, brecv_sem).wait_send()


def mixer(live, zx, bcdt, idc, idr, wx, wbc, hv):
    size = lax.axis_size("seq")
    rows = zx.shape[0] - HALO
    width = zx.shape[1] // 2
    states = wbc.shape[1] // 2
    heads_pad = hv.shape[1]
    chunks = rows // CHUNK
    slab = states // size
    vmem = pl.BlockSpec(memory_space=pltpu.VMEM)
    dma = pltpu.SemaphoreType.DMA((size - 1,))
    return pl.pallas_call(
        functools.partial(mixer_kernel, live),
        out_shape=(
            jax.ShapeDtypeStruct((rows, width), bf16),
            jax.ShapeDtypeStruct((rows, LANES), f32),
        ),
        in_specs=[vmem] * 7,
        out_specs=(vmem, vmem),
        scratch_shapes=[
            pltpu.VMEM((3, rows, LANES), f32),
            pltpu.VMEM((rows, heads_pad), f32),
            pltpu.VMEM((chunks, heads_pad, CHUNK), f32),
            pltpu.VMEM((chunks, heads_pad, CHUNK), f32),
            pltpu.VMEM((rows, 2 * heads_pad), bf16),
            pltpu.VMEM((rows, 2 * heads_pad), bf16),
            pltpu.VMEM((chunks, 8, heads_pad), f32),
            pltpu.VMEM((rows, states), bf16),
            pltpu.VMEM((rows, states), bf16),
            pltpu.VMEM((chunks, CHUNK, CHUNK), f32),
            pltpu.VMEM((rows, width), bf16),
            pltpu.VMEM((chunks, states, width), f32),
            pltpu.VMEM((rows, width), f32),
            pltpu.VMEM((size, slab, width), bf16),
            pltpu.VMEM((size, slab, width), bf16),
            pltpu.VMEM((1, width), f32),
            pltpu.VMEM((size, 1, width), f32),
            pltpu.VMEM((size, slab, width), bf16),
            pltpu.VMEM((size, slab, width), bf16),
            dma,
            dma,
            dma,
            dma,
            dma,
            dma,
        ],
        compiler_params=pltpu.CompilerParams(
            collective_id=live, has_side_effects=True, vmem_limit_bytes=56 * 1024 * 1024
        ),
        name=f"mixer_{live}",
    )(zx, bcdt, idc, idr, wx, wbc, hv)


def rms_rows(hidden_f, norm_scale):
    return (
        hidden_f
        * lax.rsqrt(jnp.mean(hidden_f * hidden_f, axis=1, keepdims=True) + epsilon)
        * norm_scale[None, :]
    ).astype(bf16)


def local(
    hidden_in,
    doc_ids,
    norm_gain,
    in_zx,
    in_bc,
    in_dt,
    conv_x,
    conv_bc,
    bias_x,
    bias_bc,
    dt_bias,
    a_log,
    d_skip,
    gated_gain,
    out_w,
):
    sections = lax.axis_size("pipe")
    section_index = lax.axis_index("pipe")
    local_width = gated_gain.shape[1]
    full_width = local_width * lax.axis_size("tp")
    heads = dt_bias.shape[1]
    head_width = local_width // heads
    heads_pad = -(-heads // LANES) * LANES
    weight_zx = in_zx[0].reshape(in_zx.shape[1], 2 * local_width)
    weight_small = jnp.concatenate(
        [in_bc[0], jnp.pad(in_dt[0], ((0, 0), (0, heads_pad - heads)))], 1
    )
    wx = jnp.concatenate(
        [
            conv_x[0],
            bias_x,
            jnp.repeat(d_skip, head_width, axis=1),
            gated_gain,
            jnp.zeros_like(gated_gain),
        ],
        0,
    )
    wbc = jnp.concatenate([conv_bc[0], bias_bc, jnp.zeros((3, bias_bc.shape[1]), f32)], 0)
    hv = jnp.pad(
        jnp.concatenate([dt_bias, -jnp.exp(a_log) * LOG2E], 0),
        ((0, 6), (0, heads_pad - heads)),
    )
    row_ids = doc_ids[0].astype(f32)
    edge = lax.ppermute(
        row_ids[-HALO:] + 1.0,
        "seq",
        [(i, i + 1) for i in range(lax.axis_size("seq") - 1)],
    )
    ids_ext = jnp.concatenate([edge - 1.0, row_ids])
    idc = jnp.broadcast_to(ids_ext[:, None], (ids_ext.shape[0], LANES))
    idr = jnp.broadcast_to(row_ids[None, :], (8, row_ids.shape[0]))
    current = hidden_in[0]
    finished = current
    for live in range(sections):
        if live > 0:
            received = lax.ppermute(finished, "pipe", [(live - 1, live)])
            current = jnp.where(section_index == live, received, current)
        current_f = current.astype(f32)
        normed = gathered_rows(rms_rows(current_f, norm_gain[0]), "tp", live)
        halo = live_shift(normed[-HALO:], "seq", 1, live)
        normed = jnp.concatenate([halo, normed], 0)
        zx = jnp.dot(normed, weight_zx, preferred_element_type=f32).astype(bf16)
        bcdt = jnp.dot(normed, weight_small, preferred_element_type=f32)
        gated, squares = mixer(live, zx, bcdt, idc, idr, wx, wbc, hv)
        part = jnp.dot(gated, out_w[0], preferred_element_type=f32)
        total, square = scattered_sum(part, jnp.sum(squares, axis=1), "tp", live)
        branch = total * lax.rsqrt(square / full_width + epsilon)[:, None]
        done = (current_f + branch).astype(bf16)
        finished = done if live == 0 else jnp.where(section_index == live, done, finished)
    return finished[None, None]


def solution(mesh):
    placed = (
        P(None, ("seq", "tp"), None),
        P(None, "seq"),
        P("pipe", None),
        P("pipe", None, None, "tp"),
        P("pipe", None, None),
        P("pipe", None, "tp"),
        P("pipe", None, "tp"),
        P("pipe", None, None),
        P("pipe", "tp"),
        P("pipe", None),
        P("pipe", "tp"),
        P("pipe", "tp"),
        P("pipe", "tp"),
        P("pipe", "tp"),
        P("pipe", "tp", None),
    )
    return jax.shard_map(
        local,
        mesh=mesh,
        in_specs=placed,
        out_specs=P("pipe", None, ("seq", "tp"), None),
        check_vma=False,
    )
```

```python
import functools

import jax
import jax.numpy as jnp
from jax import lax
from jax.experimental import pallas as pl
from jax.experimental.pallas import tpu as pltpu
from jax.sharding import PartitionSpec as P

epsilon = 1e-05
LOG2E = 1.4426950408889634
HALO = 16
CHUNK = 128
LANES = 128
MESH = pl.DeviceIdType.MESH
f32 = jnp.float32
bf16 = jnp.bfloat16


def silu(value):
    half = 0.5 * value
    return half + half * jnp.tanh(half)


def widen(value, count):
    return jnp.concatenate([value] * count, 1)


def split_pair(value):
    high = value.astype(bf16)
    low = (value - high.astype(f32)).astype(bf16)
    return jnp.concatenate([high, low], 1)


def mixer_kernel(
    live,
    zx_ref,
    bcdt_ref,
    idc_ref,
    idr_ref,
    wx_ref,
    wbc_ref,
    hv_ref,
    g_ref,
    ss_ref,
    mask_s,
    l_s,
    m_s,
    lg_s,
    ew_s,
    cw_s,
    keep_s,
    keepx_s,
    b_s,
    c_s,
    gm_s,
    xc_s,
    fresh_s,
    y_s,
    send_s,
    recv_s,
    ksend_s,
    krecv_s,
    back_s,
    inc_s,
    send_sem,
    recv_sem,
    ksend_sem,
    krecv_sem,
    bsend_sem,
    brecv_sem,
):
    size = lax.axis_size("seq")
    me = lax.axis_index("seq")
    rows = g_ref.shape[0]
    width = g_ref.shape[1]
    chunks = rows // CHUNK
    tiles = width // LANES
    states = b_s.shape[1]
    slab = states // size
    heads_pad = hv_ref.shape[1]
    head_width = LANES // 2
    group = 2 if tiles % 2 == 0 else 1
    span = group * LANES

    def lane_iota(shape):
        return lax.broadcasted_iota(jnp.int32, shape, 1)

    def row_iota(shape):
        return lax.broadcasted_iota(jnp.int32, shape, 0)

    def selector(tile, count, dtype):
        shape = (count, span)
        hit = lax.rem(row_iota(shape), heads_pad) == tile * 2 + lane_iota(shape) // head_width
        return hit.astype(f32).astype(dtype)

    def hop(source, target_ref, distance, send, recv):
        return pltpu.make_async_remote_copy(
            src_ref=source,
            dst_ref=target_ref,
            send_sem=send.at[distance - 1],
            recv_sem=recv.at[distance - 1],
            device_id={"seq": lax.rem(me + distance, size)},
            device_id_type=MESH,
        )

    @pl.when(lax.axis_index("pipe") == live)
    def _():
        barrier = pltpu.get_barrier_semaphore()
        for distance in range(1, size):
            pl.semaphore_signal(
                barrier,
                inc=1,
                device_id={"seq": lax.rem(me + distance, size)},
                device_id_type=MESH,
            )

        square_shape = (CHUNK, CHUNK)
        lower = row_iota(square_shape) >= lane_iota(square_shape)
        lower_f = lower.astype(f32)
        keep_s[...] = jnp.zeros_like(keep_s)

        @pl.loop(0, chunks)
        def _(k):
            base = pl.multiple_of(k * CHUNK, CHUNK)
            here = pl.ds(base, CHUNK)
            ids_ext = idc_ref[pl.ds(base, CHUNK + HALO), :]
            seg = ids_ext[HALO:]
            prev = ids_ext[HALO - 1 : HALO]
            last = ids_ext[HALO + CHUNK - 1 :]
            for d in range(1, 4):
                same = pltpu.roll(ids_ext, d, 0)[HALO:] == seg
                mask_s[d - 1, here, :] = same.astype(f32)
            raw = bcdt_ref[pl.ds(base + HALO, CHUNK), 2 * states :] + hv_ref[0:1, :]
            step = jnp.maximum(raw, 0.0) + jnp.log1p(jnp.exp(-jnp.abs(raw)))
            level = jnp.dot(
                lower_f,
                step * hv_ref[1:2, :],
                precision=lax.Precision.HIGHEST,
                preferred_element_type=f32,
            )
            l_s[here, :] = level
            step_log = jnp.log(step) * LOG2E
            m_s[k] = (level - step_log).T
            lg_s[k] = step_log.T
            end = level[CHUNK - 1 :]
            ew_s[here, :] = split_pair(
                jnp.exp2(end - level) * step * (seg == last).astype(f32)
            )
            cw_s[here, :] = split_pair(jnp.exp2(level) * (seg == prev).astype(f32))
            keep_s[pl.ds(k, 1), :] = jnp.exp2(end) * (last == prev).astype(f32)
            for half in range(2):
                cols = pl.ds(half * states, states)
                wide = bcdt_ref[pl.ds(base, CHUNK + HALO), cols]
                total = wbc_ref[4:5, cols] + wbc_ref[3:4, cols] * wide[HALO:]
                for d in range(1, 4):
                    total += (
                        mask_s[d - 1, here, :]
                        * wbc_ref[3 - d : 4 - d, cols]
                        * pltpu.roll(wide, d, 0)[HALO:]
                    )
                place = b_s if half == 0 else c_s
                place[here, :] = silu(total).astype(bf16)
            gram = lax.dot_general(
                c_s[here, :], b_s[here, :], (((1,), (1,)), ((), ())), preferred_element_type=f32
            )
            same_doc = seg == idr_ref[0:1, pl.ds(base, CHUNK)]
            gm_s[k] = jnp.where(lower & same_doc, gram, 0.0)

        @pl.loop(0, tiles // group)
        def _(turn):
            tile = turn * group
            lanes = pl.ds(pl.multiple_of(turn * span, span), span)
            x_lanes = pl.ds(pl.multiple_of(width + turn * span, span), span)
            pick = selector(tile, 2 * heads_pad, bf16)
            keeps = jnp.dot(split_pair(keep_s[...]), pick, preferred_element_type=f32)
            keepx_s[:, lanes] = keeps
            state = jnp.zeros((states, span), f32)
            keep_all = jnp.ones((1, span), f32)
            for k in range(chunks):
                here = pl.ds(k * CHUNK, CHUNK)
                wide = zx_ref[pl.ds(k * CHUNK, CHUNK + HALO), x_lanes].astype(f32)
                total = wx_ref[4:5, lanes] + wx_ref[3:4, lanes] * wide[HALO:]
                for d in range(1, 4):
                    total += (
                        widen(mask_s[d - 1, here, :], group)
                        * wx_ref[3 - d : 4 - d, lanes]
                        * pltpu.roll(wide, d, 0)[HALO:]
                    )
                conv = silu(total)
                xc_s[here, lanes] = conv.astype(bf16)
                weight = jnp.dot(ew_s[here, :], pick, preferred_element_type=f32)
                fresh = lax.dot_general(
                    b_s[here, :],
                    (conv * weight).astype(bf16),
                    (((0,), (0,)), ((), ())),
                    preferred_element_type=f32,
                )
                fresh_s[k, :, lanes] = fresh
                keep = keeps[k : k + 1]
                state = state * keep + fresh
                keep_all = keep_all * keep
            for part in range(size):
                send_s[part, :, lanes] = state[part * slab : (part + 1) * slab].astype(bf16)
            ksend_s[:, lanes] = keep_all

        pl.semaphore_wait(barrier, size - 1)
        for distance in range(1, size):
            target = lax.rem(me + distance, size)
            hop(send_s.at[target], recv_s.at[me], distance, send_sem, recv_sem).start()
            hop(ksend_s, krecv_s.at[me], distance, ksend_sem, krecv_sem).start()
        recv_s[me] = send_s[me]
        krecv_s[me] = ksend_s[...]

        @pl.loop(0, tiles // group)
        def _(turn):
            first_half = lane_iota((CHUNK, LANES)) < head_width
            for k in range(chunks):
                here = pl.ds(k * CHUNK, CHUNK)
                base = turn * group * 2
                level = pltpu.roll(l_s[here, :], heads_pad - base, 1)
                gram = gm_s[k]
                for i in range(group):
                    lanes = pl.ds(pl.multiple_of(turn * span + i * LANES, LANES), LANES)
                    mixes = []
                    for j in range(2 * i, 2 * i + 2):
                        shift = level[:, j : j + 1] - m_s[k, pl.ds(base + j, 1), :]
                        shift = jnp.minimum(shift, lg_s[k, pl.ds(base + j, 1), :])
                        mixes.append((jnp.exp2(shift) * gram).astype(bf16))
                    conv = xc_s[here, lanes]
                    zero = jnp.zeros_like(conv)
                    both = jnp.concatenate(
                        [jnp.where(first_half, conv, zero), jnp.where(first_half, zero, conv)], 0
                    )
                    out = jnp.dot(
                        jnp.concatenate(mixes, 1), both, preferred_element_type=f32
                    )
                    y_s[here, lanes] = out + wx_ref[5:6, lanes] * conv.astype(f32)

        for distance in range(1, size):
            source = lax.rem(me - distance + size, size)
            hop(send_s.at[me], recv_s.at[source], distance, send_sem, recv_sem).wait_recv()
            hop(ksend_s, krecv_s.at[source], distance, ksend_sem, krecv_sem).wait_recv()
        run = jnp.zeros((slab, width), f32)
        for part in range(size):
            back_s[part] = run.astype(bf16)
            if part < size - 1:
                run = run * krecv_s[part] + recv_s[part].astype(f32)
        for distance in range(1, size):
            target = lax.rem(me + distance, size)
            hop(back_s.at[target], inc_s.at[me], distance, bsend_sem, brecv_sem).start()
        inc_s[me] = back_s[me]
        for distance in range(1, size):
            source = lax.rem(me - distance + size, size)
            hop(back_s.at[me], inc_s.at[source], distance, bsend_sem, brecv_sem).wait_recv()

        ss_ref[...] = jnp.zeros_like(ss_ref)

        @pl.loop(0, tiles // group)
        def _(turn):
            lanes = pl.ds(pl.multiple_of(turn * span, span), span)
            pick = selector(turn * group, 2 * heads_pad, bf16)
            keeps = keepx_s[:, lanes]
            state = jnp.concatenate(
                [inc_s[part, :, lanes].astype(f32) for part in range(size)], 0
            )
            for k in range(chunks):
                here = pl.ds(k * CHUNK, CHUNK)
                weight = jnp.dot(cw_s[here, :], pick, preferred_element_type=f32)
                carried = jnp.dot(c_s[here, :], state.astype(bf16), preferred_element_type=f32)
                out = y_s[here, lanes] + weight * carried
                gate = zx_ref[pl.ds(k * CHUNK + HALO, CHUNK), lanes].astype(f32)
                out = out * silu(gate)
                square = out * out
                sums = square[:, :LANES]
                for i in range(1, group):
                    sums += square[:, i * LANES : (i + 1) * LANES]
                ss_ref[here, :] += sums
                g_ref[here, lanes] = (out * wx_ref[6:7, lanes]).astype(bf16)
                if k < chunks - 1:
                    state = state * keeps[k : k + 1] + fresh_s[k, :, lanes]

        for distance in range(1, size):
            target = lax.rem(me + distance, size)
            hop(send_s.at[target], recv_s.at[me], distance, send_sem, recv_sem).wait_send()
            hop(ksend_s, krecv_s.at[me], distance, ksend_sem, krecv_sem).wait_send()
            hop(back_s.at[target], inc_s.at[me], distance, bsend_sem, brecv_sem).wait_send()


def mixer(live, zx, bcdt, idc, idr, wx, wbc, hv):
    size = lax.axis_size("seq")
    rows = zx.shape[0] - HALO
    width = zx.shape[1] // 2
    states = wbc.shape[1] // 2
    heads_pad = hv.shape[1]
    chunks = rows // CHUNK
    slab = states // size
    vmem = pl.BlockSpec(memory_space=pltpu.VMEM)
    dma = pltpu.SemaphoreType.DMA((size - 1,))
    return pl.pallas_call(
        functools.partial(mixer_kernel, live),
        out_shape=(
            jax.ShapeDtypeStruct((rows, width), bf16),
            jax.ShapeDtypeStruct((rows, LANES), f32),
        ),
        in_specs=[vmem] * 7,
        out_specs=(vmem, vmem),
        scratch_shapes=[
            pltpu.VMEM((3, rows, LANES), f32),
            pltpu.VMEM((rows, heads_pad), f32),
            pltpu.VMEM((chunks, heads_pad, CHUNK), f32),
            pltpu.VMEM((chunks, heads_pad, CHUNK), f32),
            pltpu.VMEM((rows, 2 * heads_pad), bf16),
            pltpu.VMEM((rows, 2 * heads_pad), bf16),
            pltpu.VMEM((8, heads_pad), f32),
            pltpu.VMEM((8, width), f32),
            pltpu.VMEM((rows, states), bf16),
            pltpu.VMEM((rows, states), bf16),
            pltpu.VMEM((chunks, CHUNK, CHUNK), f32),
            pltpu.VMEM((rows, width), bf16),
            pltpu.VMEM((chunks, states, width), f32),
            pltpu.VMEM((rows, width), f32),
            pltpu.VMEM((size, slab, width), bf16),
            pltpu.VMEM((size, slab, width), bf16),
            pltpu.VMEM((1, width), f32),
            pltpu.VMEM((size, 1, width), f32),
            pltpu.VMEM((size, slab, width), bf16),
            pltpu.VMEM((size, slab, width), bf16),
            dma,
            dma,
            dma,
            dma,
            dma,
            dma,
        ],
        compiler_params=pltpu.CompilerParams(
            collective_id=live, has_side_effects=True, vmem_limit_bytes=56 * 1024 * 1024
        ),
        name=f"mixer_{live}",
    )(zx, bcdt, idc, idr, wx, wbc, hv)


def piece_width(features):
    return max(w for w in (512, 256, 128) if features % w == 0)


def boundary_kernel(out_live, in_live, *refs):
    refs = iter(refs)
    take = lambda count: [next(refs) for _ in range(count)]
    sends_rows = out_live is None
    if out_live is not None:
        gated_ref, squares_ref, weight_out = take(3)
    (hidden_ref,) = take(1)
    if in_live is not None:
        gain_ref, weight_zx, weight_small = take(3)
    if out_live is not None:
        (done_ref,) = take(1)
    if in_live is not None:
        zx_ref, small_ref = take(2)
    if out_live is not None:
        wo_s, part_s, psend_s, precv_s, sqsend_s, sqrecv_s = take(6)
        wo_sem, psend_sem, precv_sem, sqsend_sem, sqrecv_sem = take(5)
    if in_live is not None:
        rows_s, wz_s, acc_s, accb_s, squares_s, gain_s = take(6)
        wz_sem, rsend_sem, rrecv_sem, hsend_sem, hrecv_sem = take(5)

    tp = lax.axis_size("tp")
    shards = lax.axis_size("seq")
    t = lax.axis_index("tp")
    s = lax.axis_index("seq")
    pipe = lax.axis_index("pipe")
    count, features = hidden_ref.shape
    piece = piece_width(features)
    pieces = features // piece
    has_next = (t == tp - 1) & (s < shards - 1)
    from_live = in_live if sends_rows else out_live

    def peer(distance):
        return lax.rem(t + distance, tp)

    def cols(c):
        return pl.ds(c * piece, piece)

    def row_copy(source, c, distance):
        return pltpu.make_async_remote_copy(
            src_ref=source.at[:, cols(c)],
            dst_ref=rows_s.at[c, pl.ds(pl.multiple_of(HALO + t * count, HALO), count), :],
            send_sem=rsend_sem.at[c, distance],
            recv_sem=rrecv_sem.at[c, distance],
            device_id={"pipe": in_live, "tp": peer(distance)},
            device_id_type=MESH,
        )

    def row_arrival(c, distance):
        start = HALO + lax.rem(t - distance + tp, tp) * count
        return pltpu.make_async_remote_copy(
            src_ref=rows_s.at[c, pl.ds(0, count), :],
            dst_ref=rows_s.at[c, pl.ds(pl.multiple_of(start, HALO), count), :],
            send_sem=rsend_sem.at[c, distance],
            recv_sem=rrecv_sem.at[c, distance],
            device_id={"pipe": in_live, "tp": peer(distance)},
            device_id_type=MESH,
        )

    def halo_copy(source, c, target):
        return pltpu.make_async_remote_copy(
            src_ref=source.at[pl.ds(count - HALO, HALO), cols(c)],
            dst_ref=rows_s.at[c, pl.ds(0, HALO), :],
            send_sem=hsend_sem.at[c, target],
            recv_sem=hrecv_sem.at[c],
            device_id={"pipe": in_live, "seq": s + 1, "tp": target},
            device_id_type=MESH,
        )

    def part_copy(c, distance):
        return pltpu.make_async_remote_copy(
            src_ref=psend_s.at[c, peer(distance)],
            dst_ref=precv_s.at[c, distance - 1],
            send_sem=psend_sem.at[c, distance - 1],
            recv_sem=precv_sem.at[c, distance - 1],
            device_id={"tp": peer(distance)},
            device_id_type=MESH,
        )

    def square_copy(distance):
        return pltpu.make_async_remote_copy(
            src_ref=sqsend_s.at[peer(distance)],
            dst_ref=sqrecv_s.at[distance - 1],
            send_sem=sqsend_sem.at[distance - 1],
            recv_sem=sqrecv_sem.at[distance - 1],
            device_id={"tp": peer(distance)},
            device_id_type=MESH,
        )

    def greet(**where):
        pl.semaphore_signal(
            pltpu.get_barrier_semaphore(), inc=1, device_id=where, device_id_type=MESH
        )

    def meet(number, with_next):
        barrier = pltpu.get_barrier_semaphore()
        if not with_next:
            if number:
                pl.semaphore_wait(barrier, number)
            return

        @pl.when(has_next)
        def _():
            pl.semaphore_wait(barrier, number + tp)

        if number:

            @pl.when(jnp.logical_not(has_next))
            def _():
                pl.semaphore_wait(barrier, number)

    def weight_copy(c):
        return pltpu.make_async_copy(
            weight_zx.at[pl.ds(c * piece, piece)], wz_s.at[c % 2], wz_sem.at[c % 2]
        )

    def forward_rows(source, c):
        first = 1 if sends_rows else 0
        for distance in range(first, tp):
            row_copy(source, c, distance).start()

        @pl.when(has_next)
        def _():
            for target in range(tp):
                halo_copy(source, c, target).start()

    def drain_rows(source):
        for c in range(pieces):
            for distance in range(1 if sends_rows else 0, tp):
                row_copy(source, c, distance).wait_send()

        @pl.when(has_next)
        def _():
            for c in range(pieces):
                for target in range(tp):
                    halo_copy(source, c, target).wait_send()

    def project():
        for c in range(min(2, pieces)):
            weight_copy(c).start()
        for distance in range(1 if sends_rows else 0, tp):
            greet(pipe=from_live, tp=lax.rem(t - distance + tp, tp))

        @pl.when(s > 0)
        def _():
            greet(pipe=from_live, seq=s - 1, tp=tp - 1)

        if sends_rows:
            meet(tp - 1, True)
            for c in range(pieces):
                forward_rows(hidden_ref, c)
            for c in range(pieces):
                mine = pl.ds(pl.multiple_of(HALO + t * count, HALO), count)
                rows_s[c, mine, :] = hidden_ref[:, cols(c)]

        @pl.when(s == 0)
        def _():
            rows_s[:, pl.ds(0, HALO), :] = jnp.zeros((pieces, HALO, piece), bf16)

        total_rows = rows_s.shape[1]
        out_cols = zx_ref.shape[1]
        tile = piece_width(out_cols)
        squares_s[...] = jnp.zeros_like(squares_s)
        for c in range(pieces):
            for distance in range(1 if sends_rows else 0, tp):
                row_arrival(c, distance).wait_recv()

            @pl.when(s > 0)
            def _():
                halo_copy(hidden_ref, c, 0).wait_recv()

            weight_copy(c).wait()
            values = rows_s[c].astype(f32)
            square = values * values
            sums = square[:, :LANES]
            for i in range(1, piece // LANES):
                sums += square[:, i * LANES : (i + 1) * LANES]
            squares_s[...] += sums
            gain_s[...] = (values * gain_ref[0:1, cols(c)]).astype(bf16)
            last = c == pieces - 1
            if last:
                mean = jnp.sum(squares_s[...], axis=1, keepdims=True) / features
                squares_s[...] = jnp.broadcast_to(
                    lax.rsqrt(mean + epsilon), (total_rows, LANES)
                )
            small = jnp.dot(
                gain_s[...], weight_small[pl.ds(c * piece, piece), :], preferred_element_type=f32
            )
            if c > 0:
                small += accb_s[...]
            if last:
                small_ref[...] = small * squares_s[:, 0:1]
            else:
                accb_s[...] = small

            @pl.loop(0, out_cols // tile)
            def _(n):
                at = pl.ds(pl.multiple_of(n * tile, tile), tile)
                value = jnp.dot(
                    gain_s[...], wz_s[c % 2, :, at], preferred_element_type=f32
                )
                if c > 0:
                    value += acc_s[:, at]
                if last:
                    zx_ref[:, at] = (value * widen(squares_s[...], tile // LANES)).astype(bf16)
                else:
                    acc_s[:, at] = value

            if c + 2 < pieces:
                weight_copy(c + 2).start()
        if sends_rows:
            drain_rows(hidden_ref)

    def finish():
        for c in range(pieces):
            pltpu.make_async_copy(weight_out.at[:, cols(c)], wo_s.at[c], wo_sem.at[c]).start()
        for distance in range(1, tp):
            greet(tp=peer(distance))
        for target in range(tp):
            own = squares_ref[target * count : (target + 1) * count, :]
            sqsend_s[target] = lax.dot_general(
                jnp.ones((8, LANES), f32),
                own,
                (((1,), (1,)), ((), ())),
                precision=lax.Precision.HIGHEST,
                preferred_element_type=f32,
            )
        for c in range(pieces):
            pltpu.make_async_copy(weight_out.at[:, cols(c)], wo_s.at[c], wo_sem.at[c]).wait()
            for target in range(tp):
                value = jnp.dot(
                    gated_ref[target * count : (target + 1) * count, :],
                    wo_s[c],
                    preferred_element_type=f32,
                )
                part_s[c, target] = value
                psend_s[c, target] = value.astype(bf16)
            if c == 0:
                meet(tp - 1 if in_live is None else 2 * tp - 1, in_live is not None)
                for distance in range(1, tp):
                    square_copy(distance).start()
            for distance in range(1, tp):
                part_copy(c, distance).start()
        sums = sqsend_s[t]
        for distance in range(1, tp):
            square_copy(distance).wait_recv()
            sums += sqrecv_s[distance - 1]
        sums = lax.dot_general(
            sums,
            jnp.full((8, LANES), 0.125, f32),
            (((0,), (0,)), ((), ())),
            precision=lax.Precision.HIGHEST,
            preferred_element_type=f32,
        )
        scale = lax.rsqrt(sums / (gated_ref.shape[1] * tp) + epsilon)
        for c in range(pieces):
            total = part_s[c, t]
            for distance in range(1, tp):
                part_copy(c, distance).wait_recv()
                total += precv_s[c, distance - 1].astype(f32)
            done_ref[:, cols(c)] = (
                hidden_ref[:, cols(c)].astype(f32) + total * widen(scale, piece // LANES)
            ).astype(bf16)
            if in_live is not None:
                forward_rows(done_ref, c)
        for distance in range(1, tp):
            square_copy(distance).wait_send()
            for c in range(pieces):
                part_copy(c, distance).wait_send()
        if in_live is not None:
            drain_rows(done_ref)

    if out_live is not None:
        pl.when(pipe == out_live)(finish)
    if in_live is not None:
        pl.when(pipe == in_live)(project)


def boundary(out_live, in_live, out_args, hidden, in_args):
    tp = lax.axis_size("tp")
    count, features = hidden.shape
    piece = piece_width(features)
    pieces = features // piece
    vmem = pl.BlockSpec(memory_space=pltpu.VMEM)
    hbm = pl.BlockSpec(memory_space=pl.ANY)
    dma = pltpu.SemaphoreType.DMA
    args, specs, outs, scratch = [], [], [], []
    peers = max(1, tp - 1)
    if out_live is not None:
        args += out_args
        specs += [vmem, vmem, hbm]
    args.append(hidden)
    specs.append(vmem)
    if in_live is not None:
        args += in_args
        specs += [vmem, hbm, vmem]
    if out_live is not None:
        outs.append(jax.ShapeDtypeStruct((count, features), bf16))
        width = out_args[2].shape[0]
        scratch += [
            pltpu.VMEM((pieces, width, piece), bf16),
            pltpu.VMEM((pieces, tp, count, piece), f32),
            pltpu.VMEM((pieces, tp, count, piece), bf16),
            pltpu.VMEM((pieces, peers, count, piece), bf16),
            pltpu.VMEM((tp, 8, count), f32),
            pltpu.VMEM((peers, 8, count), f32),
            dma((pieces,)),
            dma((pieces, peers)),
            dma((pieces, peers)),
            dma((peers,)),
            dma((peers,)),
        ]
    if in_live is not None:
        rows = HALO + tp * count
        wide, small = in_args[1].shape[1], in_args[2].shape[1]
        outs += [
            jax.ShapeDtypeStruct((rows, wide), bf16),
            jax.ShapeDtypeStruct((rows, small), f32),
        ]
        scratch += [
            pltpu.VMEM((pieces, rows, piece), bf16),
            pltpu.VMEM((2, piece, wide), bf16),
            pltpu.VMEM((rows, wide), f32),
            pltpu.VMEM((rows, small), f32),
            pltpu.VMEM((rows, LANES), f32),
            pltpu.VMEM((rows, piece), bf16),
            dma((2,)),
            dma((pieces, tp)),
            dma((pieces, tp)),
            dma((pieces, tp)),
            dma((pieces,)),
        ]
    sections = lax.axis_size("pipe")
    step = 0 if out_live is None else out_live + 1
    return pl.pallas_call(
        functools.partial(boundary_kernel, out_live, in_live),
        out_shape=tuple(outs),
        in_specs=specs,
        out_specs=tuple([vmem] * len(outs)),
        scratch_shapes=scratch,
        compiler_params=pltpu.CompilerParams(
            collective_id=sections + step,
            has_side_effects=True,
            vmem_limit_bytes=63 * 1024 * 1024,
        ),
        name=f"boundary_{step}",
    )(*args)


def local(
    hidden_in,
    doc_ids,
    norm_gain,
    in_zx,
    in_bc,
    in_dt,
    conv_x,
    conv_bc,
    bias_x,
    bias_bc,
    dt_bias,
    a_log,
    d_skip,
    gated_gain,
    out_w,
):
    sections = lax.axis_size("pipe")
    section_index = lax.axis_index("pipe")
    local_width = gated_gain.shape[1]
    heads = dt_bias.shape[1]
    head_width = local_width // heads
    heads_pad = -(-heads // LANES) * LANES
    weight_zx = in_zx[0].reshape(in_zx.shape[1], 2 * local_width)
    weight_small = jnp.concatenate(
        [in_bc[0], jnp.pad(in_dt[0], ((0, 0), (0, heads_pad - heads)))], 1
    )
    wx = jnp.concatenate(
        [
            conv_x[0],
            bias_x,
            jnp.repeat(d_skip, head_width, axis=1),
            gated_gain,
            jnp.zeros_like(gated_gain),
        ],
        0,
    )
    wbc = jnp.concatenate([conv_bc[0], bias_bc, jnp.zeros((3, bias_bc.shape[1]), f32)], 0)
    hv = jnp.pad(
        jnp.concatenate([dt_bias, -jnp.exp(a_log) * LOG2E], 0),
        ((0, 6), (0, heads_pad - heads)),
    )
    row_ids = doc_ids[0].astype(f32)
    edge = lax.ppermute(
        row_ids[-HALO:] + 1.0,
        "seq",
        [(i, i + 1) for i in range(lax.axis_size("seq") - 1)],
    )
    ids_ext = jnp.concatenate([edge - 1.0, row_ids])
    idc = jnp.broadcast_to(ids_ext[:, None], (ids_ext.shape[0], LANES))
    idr = jnp.broadcast_to(row_ids[None, :], (8, row_ids.shape[0]))
    gain = jnp.broadcast_to(norm_gain, (8, norm_gain.shape[1]))
    in_args = [gain, weight_zx, weight_small]
    zx, bcdt = boundary(None, 0, None, hidden_in[0], in_args)
    current = hidden_in[0]
    finished = None
    for live in range(sections):
        gated, squares = mixer(live, zx, bcdt, idc, idr, wx, wbc, hv)
        out_args = [gated, squares, out_w[0]]
        if live + 1 < sections:
            done, zx, bcdt = boundary(live, live + 1, out_args, current, in_args)
            current = lax.ppermute(done, "pipe", [(live, live + 1)])
        else:
            (done,) = boundary(live, None, out_args, current, None)
        finished = done if live == 0 else jnp.where(section_index == live, done, finished)
    return finished[None, None]


def solution(mesh):
    placed = (
        P(None, ("seq", "tp"), None),
        P(None, "seq"),
        P("pipe", None),
        P("pipe", None, None, "tp"),
        P("pipe", None, None),
        P("pipe", None, "tp"),
        P("pipe", None, "tp"),
        P("pipe", None, None),
        P("pipe", "tp"),
        P("pipe", None),
        P("pipe", "tp"),
        P("pipe", "tp"),
        P("pipe", "tp"),
        P("pipe", "tp"),
        P("pipe", "tp", None),
    )
    return jax.shard_map(
        local,
        mesh=mesh,
        in_specs=placed,
        out_specs=P("pipe", None, ("seq", "tp"), None),
        check_vma=False,
    )
```

```python
import functools

import jax
import jax.numpy as jnp
from jax import lax
from jax.experimental import pallas as pl
from jax.experimental.pallas import tpu as pltpu
from jax.sharding import PartitionSpec as P

epsilon = 1e-05
LOG2E = 1.4426950408889634
HALO = 16
CHUNK = 128
LANES = 128
MESH = pl.DeviceIdType.MESH
f32 = jnp.float32
bf16 = jnp.bfloat16


def silu(value):
    half = 0.5 * value
    return half + half * jnp.tanh(half)


def widen(value, count):
    return jnp.concatenate([value] * count, 1)


def split_pair(value):
    high = value.astype(bf16)
    low = (value - high.astype(f32)).astype(bf16)
    return jnp.concatenate([high, low], 1)


def mixer_kernel(
    live,
    x_ref,
    bcdt_ref,
    scaled_ref,
    scale_ref,
    weight_zx,
    idc_ref,
    idr_ref,
    wx_ref,
    wbc_ref,
    hv_ref,
    g_ref,
    ss_ref,
    mask_s,
    l_s,
    m_s,
    lg_s,
    ew_s,
    cw_s,
    keep_s,
    keepx_s,
    b_s,
    c_s,
    gm_s,
    xc_s,
    fresh_s,
    y_s,
    send_s,
    recv_s,
    ksend_s,
    krecv_s,
    back_s,
    inc_s,
    rows_s,
    wz_s,
    z_s,
    rows_sem,
    wz_sem,
    send_sem,
    recv_sem,
    ksend_sem,
    krecv_sem,
    bsend_sem,
    brecv_sem,
):
    size = lax.axis_size("seq")
    me = lax.axis_index("seq")
    rows = g_ref.shape[0]
    width = g_ref.shape[1]
    chunks = rows // CHUNK
    tiles = width // LANES
    states = b_s.shape[1]
    slab = states // size
    heads_pad = hv_ref.shape[1]
    head_width = LANES // 2
    group = 2 if tiles % 2 == 0 else 1
    span = group * LANES

    def lane_iota(shape):
        return lax.broadcasted_iota(jnp.int32, shape, 1)

    def row_iota(shape):
        return lax.broadcasted_iota(jnp.int32, shape, 0)

    def selector(tile, count, dtype):
        shape = (count, span)
        hit = lax.rem(row_iota(shape), heads_pad) == tile * 2 + lane_iota(shape) // head_width
        return hit.astype(f32).astype(dtype)

    def hop(source, target_ref, distance, send, recv):
        return pltpu.make_async_remote_copy(
            src_ref=source,
            dst_ref=target_ref,
            send_sem=send.at[distance - 1],
            recv_sem=recv.at[distance - 1],
            device_id={"seq": lax.rem(me + distance, size)},
            device_id_type=MESH,
        )

    @pl.when(lax.axis_index("pipe") == live)
    def _():
        barrier = pltpu.get_barrier_semaphore()
        rows_copy = pltpu.make_async_copy(scaled_ref.at[pl.ds(HALO, rows)], rows_s, rows_sem)
        rows_copy.start()
        gate_tile = wz_s.shape[2]

        def gate_copy(n):
            return pltpu.make_async_copy(
                weight_zx.at[:, pl.ds(n * gate_tile, gate_tile)], wz_s.at[n], wz_sem.at[n]
            )

        for n in range(width // gate_tile):
            gate_copy(n).start()
        for distance in range(1, size):
            pl.semaphore_signal(
                barrier,
                inc=1,
                device_id={"seq": lax.rem(me + distance, size)},
                device_id_type=MESH,
            )

        square_shape = (CHUNK, CHUNK)
        lower = row_iota(square_shape) >= lane_iota(square_shape)
        lower_f = lower.astype(f32)
        keep_s[...] = jnp.zeros_like(keep_s)

        @pl.loop(0, chunks)
        def _(k):
            base = pl.multiple_of(k * CHUNK, CHUNK)
            here = pl.ds(base, CHUNK)
            ids_ext = idc_ref[pl.ds(base, CHUNK + HALO), :]
            seg = ids_ext[HALO:]
            prev = ids_ext[HALO - 1 : HALO]
            last = ids_ext[HALO + CHUNK - 1 :]
            for d in range(1, 4):
                same = pltpu.roll(ids_ext, d, 0)[HALO:] == seg
                mask_s[d - 1, here, :] = same.astype(f32)
            raw = bcdt_ref[pl.ds(base + HALO, CHUNK), 2 * states :] + hv_ref[0:1, :]
            step = jnp.maximum(raw, 0.0) + jnp.log1p(jnp.exp(-jnp.abs(raw)))
            level = jnp.dot(
                lower_f,
                step * hv_ref[1:2, :],
                precision=lax.Precision.HIGHEST,
                preferred_element_type=f32,
            )
            l_s[here, :] = level
            step_log = jnp.log(step) * LOG2E
            m_s[k] = (level - step_log).T
            lg_s[k] = step_log.T
            end = level[CHUNK - 1 :]
            ew_s[here, :] = split_pair(
                jnp.exp2(end - level) * step * (seg == last).astype(f32)
            )
            cw_s[here, :] = split_pair(jnp.exp2(level) * (seg == prev).astype(f32))
            keep_s[pl.ds(k, 1), :] = jnp.exp2(end) * (last == prev).astype(f32)
            for half in range(2):
                cols = pl.ds(half * states, states)
                wide = bcdt_ref[pl.ds(base, CHUNK + HALO), cols]
                total = wbc_ref[4:5, cols] + wbc_ref[3:4, cols] * wide[HALO:]
                for d in range(1, 4):
                    total += (
                        mask_s[d - 1, here, :]
                        * wbc_ref[3 - d : 4 - d, cols]
                        * pltpu.roll(wide, d, 0)[HALO:]
                    )
                place = b_s if half == 0 else c_s
                place[here, :] = silu(total).astype(bf16)
            gram = lax.dot_general(
                c_s[here, :], b_s[here, :], (((1,), (1,)), ((), ())), preferred_element_type=f32
            )
            same_doc = seg == idr_ref[0:1, pl.ds(base, CHUNK)]
            gm_s[k] = jnp.where(lower & same_doc, gram, 0.0)

        @pl.loop(0, tiles // group)
        def _(turn):
            tile = turn * group
            lanes = pl.ds(pl.multiple_of(turn * span, span), span)
            pick = selector(tile, 2 * heads_pad, bf16)
            keeps = jnp.dot(split_pair(keep_s[...]), pick, preferred_element_type=f32)
            keepx_s[:, lanes] = keeps
            state = jnp.zeros((states, span), f32)
            keep_all = jnp.ones((1, span), f32)
            for k in range(chunks):
                here = pl.ds(k * CHUNK, CHUNK)
                wide = x_ref[pl.ds(k * CHUNK, CHUNK + HALO), lanes].astype(f32)
                total = wx_ref[4:5, lanes] + wx_ref[3:4, lanes] * wide[HALO:]
                for d in range(1, 4):
                    total += (
                        widen(mask_s[d - 1, here, :], group)
                        * wx_ref[3 - d : 4 - d, lanes]
                        * pltpu.roll(wide, d, 0)[HALO:]
                    )
                conv = silu(total)
                xc_s[here, lanes] = conv.astype(bf16)
                weight = jnp.dot(ew_s[here, :], pick, preferred_element_type=f32)
                fresh = lax.dot_general(
                    b_s[here, :],
                    (conv * weight).astype(bf16),
                    (((0,), (0,)), ((), ())),
                    preferred_element_type=f32,
                )
                fresh_s[k, :, lanes] = fresh
                keep = keeps[k : k + 1]
                state = state * keep + fresh
                keep_all = keep_all * keep
            for part in range(size):
                send_s[part, :, lanes] = state[part * slab : (part + 1) * slab].astype(bf16)
            ksend_s[:, lanes] = keep_all

        pl.semaphore_wait(barrier, size - 1)
        for distance in range(1, size):
            target = lax.rem(me + distance, size)
            hop(send_s.at[target], recv_s.at[me], distance, send_sem, recv_sem).start()
            hop(ksend_s, krecv_s.at[me], distance, ksend_sem, krecv_sem).start()
        recv_s[me] = send_s[me]
        krecv_s[me] = ksend_s[...]

        @pl.loop(0, tiles // group)
        def _(turn):
            first_half = lane_iota((CHUNK, LANES)) < head_width
            for k in range(chunks):
                here = pl.ds(k * CHUNK, CHUNK)
                base = turn * group * 2
                level = pltpu.roll(l_s[here, :], heads_pad - base, 1)
                gram = gm_s[k]
                for i in range(group):
                    lanes = pl.ds(pl.multiple_of(turn * span + i * LANES, LANES), LANES)
                    mixes = []
                    for j in range(2 * i, 2 * i + 2):
                        shift = level[:, j : j + 1] - m_s[k, pl.ds(base + j, 1), :]
                        shift = jnp.minimum(shift, lg_s[k, pl.ds(base + j, 1), :])
                        mixes.append((jnp.exp2(shift) * gram).astype(bf16))
                    conv = xc_s[here, lanes]
                    zero = jnp.zeros_like(conv)
                    both = jnp.concatenate(
                        [jnp.where(first_half, conv, zero), jnp.where(first_half, zero, conv)], 0
                    )
                    out = jnp.dot(
                        jnp.concatenate(mixes, 1), both, preferred_element_type=f32
                    )
                    y_s[here, lanes] = out + wx_ref[5:6, lanes] * conv.astype(f32)

        for distance in range(1, size):
            source = lax.rem(me - distance + size, size)
            hop(send_s.at[me], recv_s.at[source], distance, send_sem, recv_sem).wait_recv()
            hop(ksend_s, krecv_s.at[source], distance, ksend_sem, krecv_sem).wait_recv()
        run = jnp.zeros((slab, width), f32)
        for part in range(size):
            back_s[part] = run.astype(bf16)
            if part < size - 1:
                run = run * krecv_s[part] + recv_s[part].astype(f32)
        for distance in range(1, size):
            target = lax.rem(me + distance, size)
            hop(back_s.at[target], inc_s.at[me], distance, bsend_sem, brecv_sem).start()
        inc_s[me] = back_s[me]
        rows_copy.wait()
        for n in range(width // gate_tile):
            gate_copy(n).wait()

        @pl.loop(0, width // gate_tile)
        def _(n):
            at = pl.ds(pl.multiple_of(n * gate_tile, gate_tile), gate_tile)
            gate = jnp.dot(rows_s[...], wz_s[n], preferred_element_type=f32)
            z_s[:, at] = (
                gate * widen(scale_ref[pl.ds(HALO, rows), :], gate_tile // LANES)
            ).astype(bf16)

        for distance in range(1, size):
            source = lax.rem(me - distance + size, size)
            hop(back_s.at[me], inc_s.at[source], distance, bsend_sem, brecv_sem).wait_recv()

        ss_ref[...] = jnp.zeros_like(ss_ref)

        @pl.loop(0, tiles // group)
        def _(turn):
            lanes = pl.ds(pl.multiple_of(turn * span, span), span)
            pick = selector(turn * group, 2 * heads_pad, bf16)
            keeps = keepx_s[:, lanes]
            state = jnp.concatenate(
                [inc_s[part, :, lanes].astype(f32) for part in range(size)], 0
            )
            for k in range(chunks):
                here = pl.ds(k * CHUNK, CHUNK)
                weight = jnp.dot(cw_s[here, :], pick, preferred_element_type=f32)
                carried = jnp.dot(c_s[here, :], state.astype(bf16), preferred_element_type=f32)
                out = y_s[here, lanes] + weight * carried
                gate = z_s[here, lanes].astype(f32)
                out = out * silu(gate)
                square = out * out
                sums = square[:, :LANES]
                for i in range(1, group):
                    sums += square[:, i * LANES : (i + 1) * LANES]
                ss_ref[here, :] += sums
                g_ref[here, lanes] = (out * wx_ref[6:7, lanes]).astype(bf16)
                if k < chunks - 1:
                    state = state * keeps[k : k + 1] + fresh_s[k, :, lanes]

        for distance in range(1, size):
            target = lax.rem(me + distance, size)
            hop(send_s.at[target], recv_s.at[me], distance, send_sem, recv_sem).wait_send()
            hop(ksend_s, krecv_s.at[me], distance, ksend_sem, krecv_sem).wait_send()
            hop(back_s.at[target], inc_s.at[me], distance, bsend_sem, brecv_sem).wait_send()


def mixer(live, x_raw, bcdt, scaled, scale, weight_zx, idc, idr, wx, wbc, hv):
    size = lax.axis_size("seq")
    rows = x_raw.shape[0] - HALO
    width = x_raw.shape[1]
    features = scaled.shape[1]
    gate_tile = min(piece_width(width), 256)
    hbm = pl.BlockSpec(memory_space=pl.ANY)
    states = wbc.shape[1] // 2
    heads_pad = hv.shape[1]
    chunks = rows // CHUNK
    slab = states // size
    vmem = pl.BlockSpec(memory_space=pltpu.VMEM)
    dma = pltpu.SemaphoreType.DMA((size - 1,))
    return pl.pallas_call(
        functools.partial(mixer_kernel, live),
        out_shape=(
            jax.ShapeDtypeStruct((rows, width), bf16),
            jax.ShapeDtypeStruct((rows, LANES), f32),
        ),
        in_specs=[vmem, vmem, hbm, vmem, hbm] + [vmem] * 5,
        out_specs=(vmem, vmem),
        scratch_shapes=[
            pltpu.VMEM((3, rows, LANES), f32),
            pltpu.VMEM((rows, heads_pad), f32),
            pltpu.VMEM((chunks, heads_pad, CHUNK), f32),
            pltpu.VMEM((chunks, heads_pad, CHUNK), f32),
            pltpu.VMEM((rows, 2 * heads_pad), bf16),
            pltpu.VMEM((rows, 2 * heads_pad), bf16),
            pltpu.VMEM((8, heads_pad), f32),
            pltpu.VMEM((8, width), f32),
            pltpu.VMEM((rows, states), bf16),
            pltpu.VMEM((rows, states), bf16),
            pltpu.VMEM((chunks, CHUNK, CHUNK), f32),
            pltpu.VMEM((rows, width), bf16),
            pltpu.VMEM((chunks, states, width), f32),
            pltpu.VMEM((rows, width), f32),
            pltpu.VMEM((size, slab, width), bf16),
            pltpu.VMEM((size, slab, width), bf16),
            pltpu.VMEM((1, width), f32),
            pltpu.VMEM((size, 1, width), f32),
            pltpu.VMEM((size, slab, width), bf16),
            pltpu.VMEM((size, slab, width), bf16),
            pltpu.VMEM((rows, features), bf16),
            pltpu.VMEM((width // gate_tile, features, gate_tile), bf16),
            pltpu.VMEM((rows, width), bf16),
            pltpu.SemaphoreType.DMA,
            pltpu.SemaphoreType.DMA((width // gate_tile,)),
            dma,
            dma,
            dma,
            dma,
            dma,
            dma,
        ],
        compiler_params=pltpu.CompilerParams(
            collective_id=live, has_side_effects=True, vmem_limit_bytes=63 * 1024 * 1024
        ),
        name=f"mixer_{live}",
    )(x_raw, bcdt, scaled, scale, weight_zx, idc, idr, wx, wbc, hv)


def piece_width(features):
    return max(w for w in (512, 256, 128) if features % w == 0)


def boundary_kernel(out_live, in_live, *refs):
    refs = iter(refs)
    take = lambda count: [next(refs) for _ in range(count)]
    sends_rows = out_live is None
    if out_live is not None:
        gated_ref, squares_ref, weight_out = take(3)
    (hidden_ref,) = take(1)
    if in_live is not None:
        gain_ref, weight_zx, weight_bc, weight_dt = take(4)
    if out_live is not None:
        (done_ref,) = take(1)
    if in_live is not None:
        x_ref, small_ref, scaled_ref, scale_ref = take(4)
    if out_live is not None:
        wo_s, part_s, psend_s, precv_s, sqsend_s, sqrecv_s = take(6)
        wo_sem, psend_sem, precv_sem, sqsend_sem, sqrecv_sem = take(5)
    if in_live is not None:
        rows_s, wz_s, acc_s, accb_s, squares_s = take(5)
        wz_sem, rsend_sem, rrecv_sem, hsend_sem, hrecv_sem = take(5)

    tp = lax.axis_size("tp")
    shards = lax.axis_size("seq")
    t = lax.axis_index("tp")
    s = lax.axis_index("seq")
    pipe = lax.axis_index("pipe")
    count, features = hidden_ref.shape
    piece = piece_width(features)
    pieces = features // piece
    has_next = (t == tp - 1) & (s < shards - 1)
    from_live = in_live if sends_rows else out_live

    def peer(distance):
        return lax.rem(t + distance, tp)

    def cols(c):
        return pl.ds(c * piece, piece)

    def row_copy(source, c, distance):
        return pltpu.make_async_remote_copy(
            src_ref=source.at[:, cols(c)],
            dst_ref=rows_s.at[c, pl.ds(pl.multiple_of(HALO + t * count, HALO), count), :],
            send_sem=rsend_sem.at[c, distance],
            recv_sem=rrecv_sem.at[c, distance],
            device_id={"pipe": in_live, "tp": peer(distance)},
            device_id_type=MESH,
        )

    def row_arrival(c, distance):
        start = HALO + lax.rem(t - distance + tp, tp) * count
        return pltpu.make_async_remote_copy(
            src_ref=rows_s.at[c, pl.ds(0, count), :],
            dst_ref=rows_s.at[c, pl.ds(pl.multiple_of(start, HALO), count), :],
            send_sem=rsend_sem.at[c, distance],
            recv_sem=rrecv_sem.at[c, distance],
            device_id={"pipe": in_live, "tp": peer(distance)},
            device_id_type=MESH,
        )

    def halo_copy(source, c, target):
        return pltpu.make_async_remote_copy(
            src_ref=source.at[pl.ds(count - HALO, HALO), cols(c)],
            dst_ref=rows_s.at[c, pl.ds(0, HALO), :],
            send_sem=hsend_sem.at[c, target],
            recv_sem=hrecv_sem.at[c],
            device_id={"pipe": in_live, "seq": s + 1, "tp": target},
            device_id_type=MESH,
        )

    def part_copy(c, distance):
        return pltpu.make_async_remote_copy(
            src_ref=psend_s.at[c, peer(distance)],
            dst_ref=precv_s.at[c, distance - 1],
            send_sem=psend_sem.at[c, distance - 1],
            recv_sem=precv_sem.at[c, distance - 1],
            device_id={"tp": peer(distance)},
            device_id_type=MESH,
        )

    def square_copy(distance):
        return pltpu.make_async_remote_copy(
            src_ref=sqsend_s.at[peer(distance)],
            dst_ref=sqrecv_s.at[distance - 1],
            send_sem=sqsend_sem.at[distance - 1],
            recv_sem=sqrecv_sem.at[distance - 1],
            device_id={"tp": peer(distance)},
            device_id_type=MESH,
        )

    def greet(**where):
        pl.semaphore_signal(
            pltpu.get_barrier_semaphore(), inc=1, device_id=where, device_id_type=MESH
        )

    def meet(number, with_next):
        barrier = pltpu.get_barrier_semaphore()
        if not with_next:
            if number:
                pl.semaphore_wait(barrier, number)
            return

        @pl.when(has_next)
        def _():
            pl.semaphore_wait(barrier, number + tp)

        if number:

            @pl.when(jnp.logical_not(has_next))
            def _():
                pl.semaphore_wait(barrier, number)

    def weight_copy(c):
        return pltpu.make_async_copy(
            weight_zx.at[pl.ds(c * piece, piece), pl.ds(x_ref.shape[1], x_ref.shape[1])],
            wz_s.at[c],
            wz_sem.at[c],
        )

    def forward_rows(source, c):
        first = 1 if sends_rows else 0
        for distance in range(first, tp):
            row_copy(source, c, distance).start()

        @pl.when(has_next)
        def _():
            for target in range(tp):
                halo_copy(source, c, target).start()

    def drain_rows(source):
        for c in range(pieces):
            for distance in range(1 if sends_rows else 0, tp):
                row_copy(source, c, distance).wait_send()

        @pl.when(has_next)
        def _():
            for c in range(pieces):
                for target in range(tp):
                    halo_copy(source, c, target).wait_send()

    def project():
        for c in range(pieces):
            weight_copy(c).start()
        for distance in range(1 if sends_rows else 0, tp):
            greet(pipe=from_live, tp=lax.rem(t - distance + tp, tp))

        @pl.when(s > 0)
        def _():
            greet(pipe=from_live, seq=s - 1, tp=tp - 1)

        if sends_rows:
            meet(tp - 1, True)
            for c in range(pieces):
                forward_rows(hidden_ref, c)
            for c in range(pieces):
                mine = pl.ds(pl.multiple_of(HALO + t * count, HALO), count)
                rows_s[c, mine, :] = hidden_ref[:, cols(c)]

        @pl.when(s == 0)
        def _():
            rows_s[:, pl.ds(0, HALO), :] = jnp.zeros((pieces, HALO, piece), bf16)

        total_rows = rows_s.shape[1]
        out_cols = x_ref.shape[1]
        tile = piece_width(out_cols)
        squares_s[...] = jnp.zeros_like(squares_s)
        for c in range(pieces):
            for distance in range(1 if sends_rows else 0, tp):
                row_arrival(c, distance).wait_recv()

            @pl.when(s > 0)
            def _():
                halo_copy(hidden_ref, c, 0).wait_recv()

            weight_copy(c).wait()
            values = rows_s[c].astype(f32)
            square = values * values
            sums = square[:, :LANES]
            for i in range(1, piece // LANES):
                sums += square[:, i * LANES : (i + 1) * LANES]
            squares_s[...] += sums
            scaled_ref[:, cols(c)] = (values * gain_ref[0:1, cols(c)]).astype(bf16)
            last = c == pieces - 1
            if last:
                mean = jnp.sum(squares_s[...], axis=1, keepdims=True) / features
                scale_ref[...] = jnp.broadcast_to(
                    lax.rsqrt(mean + epsilon), (total_rows, LANES)
                )
            start = 0
            for weight in (weight_bc, weight_dt):
                at = slice(start, start + weight.shape[1])
                start += weight.shape[1]
                small = jnp.dot(
                    scaled_ref[:, cols(c)],
                    weight[pl.ds(c * piece, piece), :],
                    preferred_element_type=f32,
                )
                if c > 0:
                    small += accb_s[:, at]
                if last:
                    small_ref[:, at] = small * widen(scale_ref[...], small.shape[1] // LANES)
                else:
                    accb_s[:, at] = small

            @pl.loop(0, out_cols // tile)
            def _(n):
                at = pl.ds(pl.multiple_of(n * tile, tile), tile)
                value = jnp.dot(
                    scaled_ref[:, cols(c)], wz_s[c, :, at], preferred_element_type=f32
                )
                if c > 0:
                    value += acc_s[:, at]
                if last:
                    x_ref[:, at] = (value * widen(scale_ref[...], tile // LANES)).astype(bf16)
                else:
                    acc_s[:, at] = value

            if not sends_rows:
                mine = pl.ds(pl.multiple_of(HALO + t * count, HALO), count)
                done_ref[:, cols(c)] = rows_s[c, mine, :]
        if sends_rows:
            drain_rows(hidden_ref)

    def finish():
        for c in range(pieces):
            pltpu.make_async_copy(weight_out.at[:, cols(c)], wo_s.at[c], wo_sem.at[c]).start()
        for distance in range(1, tp):
            greet(tp=peer(distance))
        for target in range(tp):
            own = squares_ref[target * count : (target + 1) * count, :]
            sqsend_s[target] = lax.dot_general(
                jnp.ones((8, LANES), f32),
                own,
                (((1,), (1,)), ((), ())),
                precision=lax.Precision.HIGHEST,
                preferred_element_type=f32,
            )
        for c in range(pieces):
            pltpu.make_async_copy(weight_out.at[:, cols(c)], wo_s.at[c], wo_sem.at[c]).wait()
            for target in range(tp):
                value = jnp.dot(
                    gated_ref[target * count : (target + 1) * count, :],
                    wo_s[c],
                    preferred_element_type=f32,
                )
                part_s[c, target] = value
                psend_s[c, target] = value.astype(bf16)
            if c == 0:
                meet(tp - 1 if in_live is None else 2 * tp - 1, in_live is not None)
                for distance in range(1, tp):
                    square_copy(distance).start()
            for distance in range(1, tp):
                part_copy(c, distance).start()
        sums = sqsend_s[t]
        for distance in range(1, tp):
            square_copy(distance).wait_recv()
            sums += sqrecv_s[distance - 1]
        sums = lax.dot_general(
            sums,
            jnp.full((8, LANES), 0.125, f32),
            (((0,), (0,)), ((), ())),
            precision=lax.Precision.HIGHEST,
            preferred_element_type=f32,
        )
        scale = lax.rsqrt(sums / (gated_ref.shape[1] * tp) + epsilon)
        for c in range(pieces):
            total = part_s[c, t]
            for distance in range(1, tp):
                part_copy(c, distance).wait_recv()
                total += precv_s[c, distance - 1].astype(f32)
            done_ref[:, cols(c)] = (
                hidden_ref[:, cols(c)].astype(f32) + total * widen(scale, piece // LANES)
            ).astype(bf16)
            if in_live is not None:
                forward_rows(done_ref, c)
        for distance in range(1, tp):
            square_copy(distance).wait_send()
            for c in range(pieces):
                part_copy(c, distance).wait_send()
        if in_live is not None:
            drain_rows(done_ref)

    if out_live is not None:
        pl.when(pipe == out_live)(finish)
    if in_live is not None:
        pl.when(pipe == in_live)(project)
    if out_live is not None:
        idle = pipe != out_live
        if in_live is not None:
            idle = idle & (pipe != in_live)

        @pl.when(idle)
        def _():
            done_ref[...] = hidden_ref[...]


def boundary(out_live, in_live, out_args, hidden, in_args):
    tp = lax.axis_size("tp")
    count, features = hidden.shape
    piece = piece_width(features)
    pieces = features // piece
    vmem = pl.BlockSpec(memory_space=pltpu.VMEM)
    hbm = pl.BlockSpec(memory_space=pl.ANY)
    dma = pltpu.SemaphoreType.DMA
    args, specs, outs, scratch = [], [], [], []
    peers = max(1, tp - 1)
    if out_live is not None:
        args += out_args
        specs += [vmem, vmem, hbm]
    args.append(hidden)
    specs.append(vmem)
    if in_live is not None:
        args += in_args
        specs += [vmem, hbm, vmem, vmem]
    if out_live is not None:
        outs.append(jax.ShapeDtypeStruct((count, features), bf16))
        width = out_args[2].shape[0]
        scratch += [
            pltpu.VMEM((pieces, width, piece), bf16),
            pltpu.VMEM((pieces, tp, count, piece), f32),
            pltpu.VMEM((pieces, tp, count, piece), bf16),
            pltpu.VMEM((pieces, peers, count, piece), bf16),
            pltpu.VMEM((tp, 8, count), f32),
            pltpu.VMEM((peers, 8, count), f32),
            dma((pieces,)),
            dma((pieces, peers)),
            dma((pieces, peers)),
            dma((peers,)),
            dma((peers,)),
        ]
    if in_live is not None:
        rows = HALO + tp * count
        wide = in_args[1].shape[1] // 2
        small = in_args[2].shape[1] + in_args[3].shape[1]
        outs += [
            jax.ShapeDtypeStruct((rows, wide), bf16),
            jax.ShapeDtypeStruct((rows, small), f32),
            jax.ShapeDtypeStruct((rows, features), bf16),
            jax.ShapeDtypeStruct((rows, LANES), f32),
        ]
        scratch += [
            pltpu.VMEM((pieces, rows, piece), bf16),
            pltpu.VMEM((pieces, piece, wide), bf16),
            pltpu.VMEM((rows, wide), f32),
            pltpu.VMEM((rows, small), f32),
            pltpu.VMEM((rows, LANES), f32),
            dma((pieces,)),
            dma((pieces, tp)),
            dma((pieces, tp)),
            dma((pieces, tp)),
            dma((pieces,)),
        ]
    sections = lax.axis_size("pipe")
    step = 0 if out_live is None else out_live + 1
    return pl.pallas_call(
        functools.partial(boundary_kernel, out_live, in_live),
        out_shape=tuple(outs),
        in_specs=specs,
        out_specs=tuple([vmem] * len(outs)),
        scratch_shapes=scratch,
        compiler_params=pltpu.CompilerParams(
            collective_id=sections + step,
            has_side_effects=True,
            vmem_limit_bytes=63 * 1024 * 1024,
        ),
        name=f"boundary_{step}",
    )(*args)


def local(
    hidden_in,
    doc_ids,
    norm_gain,
    in_zx,
    in_bc,
    in_dt,
    conv_x,
    conv_bc,
    bias_x,
    bias_bc,
    dt_bias,
    a_log,
    d_skip,
    gated_gain,
    out_w,
):
    sections = lax.axis_size("pipe")
    local_width = gated_gain.shape[1]
    heads = dt_bias.shape[1]
    head_width = local_width // heads
    heads_pad = -(-heads // LANES) * LANES
    weight_zx = in_zx[0].reshape(in_zx.shape[1], 2 * local_width)
    weight_dt = jnp.pad(in_dt[0], ((0, 0), (0, heads_pad - heads)))
    wx = jnp.concatenate(
        [
            conv_x[0],
            bias_x,
            jnp.repeat(d_skip, head_width, axis=1),
            gated_gain,
            jnp.zeros_like(gated_gain),
        ],
        0,
    )
    wbc = jnp.concatenate([conv_bc[0], bias_bc, jnp.zeros((3, bias_bc.shape[1]), f32)], 0)
    hv = jnp.pad(
        jnp.concatenate([dt_bias, -jnp.exp(a_log) * LOG2E], 0),
        ((0, 6), (0, heads_pad - heads)),
    )
    row_ids = doc_ids[0].astype(f32)
    edge = lax.ppermute(
        row_ids[-HALO:] + 1.0,
        "seq",
        [(i, i + 1) for i in range(lax.axis_size("seq") - 1)],
    )
    ids_ext = jnp.concatenate([edge - 1.0, row_ids])
    idc = jnp.broadcast_to(ids_ext[:, None], (ids_ext.shape[0], LANES))
    idr = jnp.broadcast_to(row_ids[None, :], (8, row_ids.shape[0]))
    gain = jnp.broadcast_to(norm_gain, (8, norm_gain.shape[1]))
    in_args = [gain, weight_zx, in_bc[0], weight_dt]
    projected = boundary(None, 0, None, hidden_in[0], in_args)
    current = hidden_in[0]
    for live in range(sections):
        gated, squares = mixer(live, *projected, weight_zx, idc, idr, wx, wbc, hv)
        out_args = [gated, squares, out_w[0]]
        if live + 1 < sections:
            current, *projected = boundary(live, live + 1, out_args, current, in_args)
        else:
            (current,) = boundary(live, None, out_args, current, None)
    return current[None, None]


def solution(mesh):
    placed = (
        P(None, ("seq", "tp"), None),
        P(None, "seq"),
        P("pipe", None),
        P("pipe", None, None, "tp"),
        P("pipe", None, None),
        P("pipe", None, "tp"),
        P("pipe", None, "tp"),
        P("pipe", None, None),
        P("pipe", "tp"),
        P("pipe", None),
        P("pipe", "tp"),
        P("pipe", "tp"),
        P("pipe", "tp"),
        P("pipe", "tp"),
        P("pipe", "tp", None),
    )
    return jax.shard_map(
        local,
        mesh=mesh,
        in_specs=placed,
        out_specs=P("pipe", None, ("seq", "tp"), None),
        check_vma=False,
    )
```

```python
import functools

import jax
import jax.numpy as jnp
from jax import lax
from jax.experimental import pallas as pl
from jax.experimental.pallas import tpu as pltpu
from jax.sharding import PartitionSpec as P

epsilon = 1e-05
LOG2E = 1.4426950408889634
HALO = 16
CHUNK = 128
LANES = 128
MESH = pl.DeviceIdType.MESH
f32 = jnp.float32
bf16 = jnp.bfloat16


def silu(value):
    half = 0.5 * value
    return half + half * jnp.tanh(half)


def widen(value, count):
    return jnp.concatenate([value] * count, 1)


def split_pair(value):
    high = value.astype(bf16)
    low = (value - high.astype(f32)).astype(bf16)
    return jnp.concatenate([high, low], 1)


def mixer_kernel(
    live,
    x_ref,
    bcdt_ref,
    scaled_ref,
    scale_ref,
    weight_zx,
    idc_ref,
    idr_ref,
    cx_ref,
    bx_ref,
    gg_ref,
    cb_ref,
    bb_ref,
    hv_ref,
    g_ref,
    ss_ref,
    mask_s,
    l_s,
    m_s,
    lg_s,
    ew_s,
    cw_s,
    keep_s,
    keepx_s,
    b_s,
    c_s,
    gm_s,
    xc_s,
    fresh_s,
    y_s,
    send_s,
    recv_s,
    ksend_s,
    krecv_s,
    back_s,
    inc_s,
    rows_s,
    wz_s,
    z_s,
    rows_sem,
    wz_sem,
    send_sem,
    recv_sem,
    ksend_sem,
    krecv_sem,
    bsend_sem,
    brecv_sem,
):
    size = lax.axis_size("seq")
    me = lax.axis_index("seq")
    rows = g_ref.shape[0]
    width = g_ref.shape[1]
    chunks = rows // CHUNK
    tiles = width // LANES
    states = b_s.shape[1]
    slab = states // size
    heads_pad = hv_ref.shape[1]
    head_width = LANES // 2
    group = 2 if tiles % 2 == 0 else 1
    span = group * LANES

    def lane_iota(shape):
        return lax.broadcasted_iota(jnp.int32, shape, 1)

    def row_iota(shape):
        return lax.broadcasted_iota(jnp.int32, shape, 0)

    def selector(tile, count, dtype):
        shape = (count, span)
        hit = lax.rem(row_iota(shape), heads_pad) == tile * 2 + lane_iota(shape) // head_width
        return hit.astype(f32).astype(dtype)

    turns = tiles // group
    middle = turns // 2
    halves = [(0, middle), (middle, turns)]
    cuts = [0, turns * 3 // 10, turns * 6 // 10, turns]

    def hop(source, target_ref, half, distance, send, recv):
        first, end = halves[half]
        cols = pl.ds(first * span, (end - first) * span)
        return pltpu.make_async_remote_copy(
            src_ref=source.at[:, cols],
            dst_ref=target_ref.at[:, cols],
            send_sem=send.at[half, distance - 1],
            recv_sem=recv.at[half, distance - 1],
            device_id={"seq": lax.rem(me + distance, size)},
            device_id_type=MESH,
        )

    @pl.when(lax.axis_index("pipe") == live)
    def _():
        barrier = pltpu.get_barrier_semaphore()
        rows_copy = pltpu.make_async_copy(scaled_ref.at[pl.ds(HALO, rows)], rows_s, rows_sem)
        rows_copy.start()
        gate_tile = span

        def gate_copy(n):
            return pltpu.make_async_copy(
                weight_zx.at[:, pl.ds(n * gate_tile, gate_tile)], wz_s.at[n], wz_sem.at[n]
            )

        for n in range(width // gate_tile):
            gate_copy(n).start()
        for distance in range(1, size):
            pl.semaphore_signal(
                barrier,
                inc=1,
                device_id={"seq": lax.rem(me + distance, size)},
                device_id_type=MESH,
            )

        square_shape = (CHUNK, CHUNK)
        lower = row_iota(square_shape) >= lane_iota(square_shape)
        lower_f = lower.astype(f32)
        keep_s[...] = jnp.zeros_like(keep_s)
        keep_s[chunks : chunks + 1, :] = hv_ref[2:3, :]
        rate = jnp.exp(hv_ref[1:2, :]) * -LOG2E

        @pl.loop(0, chunks)
        def _(k):
            base = pl.multiple_of(k * CHUNK, CHUNK)
            here = pl.ds(base, CHUNK)
            ids_ext = idc_ref[pl.ds(base, CHUNK + HALO), :]
            seg = ids_ext[HALO:]
            prev = ids_ext[HALO - 1 : HALO]
            last = ids_ext[HALO + CHUNK - 1 :]
            for d in range(1, 4):
                same = pltpu.roll(ids_ext, d, 0)[HALO:] == seg
                mask_s[d - 1, here, :] = same.astype(f32)
            raw = bcdt_ref[pl.ds(base + HALO, CHUNK), 2 * states :] + hv_ref[0:1, :]
            step = jnp.maximum(raw, 0.0) + jnp.log1p(jnp.exp(-jnp.abs(raw)))
            level = jnp.dot(
                lower_f,
                step * rate,
                precision=lax.Precision.HIGHEST,
                preferred_element_type=f32,
            )
            l_s[here, :] = level
            step_log = jnp.log(step) * LOG2E
            m_s[k] = (level - step_log).T
            lg_s[k] = step_log.T
            end = level[CHUNK - 1 :]
            ew_s[here, :] = split_pair(
                jnp.exp2(end - level) * step * (seg == last).astype(f32)
            )
            cw_s[here, :] = split_pair(jnp.exp2(level) * (seg == prev).astype(f32))
            keep_s[pl.ds(k, 1), :] = jnp.exp2(end) * (last == prev).astype(f32)
            for half in range(2):
                cols = pl.ds(half * states, states)
                wide = bcdt_ref[pl.ds(base, CHUNK + HALO), cols]
                total = bb_ref[0:1, cols] + cb_ref[3:4, cols] * wide[HALO:]
                for d in range(1, 4):
                    total += (
                        mask_s[d - 1, here, :]
                        * cb_ref[3 - d : 4 - d, cols]
                        * pltpu.roll(wide, d, 0)[HALO:]
                    )
                place = b_s if half == 0 else c_s
                place[here, :] = silu(total).astype(bf16)
            gram = lax.dot_general(
                c_s[here, :], b_s[here, :], (((1,), (1,)), ((), ())), preferred_element_type=f32
            )
            same_doc = seg == idr_ref[0:1, pl.ds(base, CHUNK)]
            gm_s[k] = jnp.where(lower & same_doc, gram, 0.0)

        def enter(turn):
            tile = turn * group
            lanes = pl.ds(pl.multiple_of(turn * span, span), span)
            pick = selector(tile, 2 * heads_pad, bf16)
            keeps = jnp.dot(split_pair(keep_s[...]), pick, preferred_element_type=f32)
            keepx_s[:, lanes] = keeps
            state = jnp.zeros((states, span), f32)
            keep_all = jnp.ones((1, span), f32)
            for k in range(chunks):
                here = pl.ds(k * CHUNK, CHUNK)
                wide = x_ref[pl.ds(k * CHUNK, CHUNK + HALO), lanes].astype(f32)
                total = bx_ref[0:1, lanes] + cx_ref[3:4, lanes] * wide[HALO:]
                for d in range(1, 4):
                    total += (
                        widen(mask_s[d - 1, here, :], group)
                        * cx_ref[3 - d : 4 - d, lanes]
                        * pltpu.roll(wide, d, 0)[HALO:]
                    )
                conv = silu(total)
                xc_s[here, lanes] = conv.astype(bf16)
                weight = jnp.dot(ew_s[here, :], pick, preferred_element_type=f32)
                fresh = lax.dot_general(
                    b_s[here, :],
                    (conv * weight).astype(bf16),
                    (((0,), (0,)), ((), ())),
                    preferred_element_type=f32,
                )
                fresh_s[k, :, lanes] = fresh
                keep = keeps[k : k + 1]
                state = state * keep + fresh
                keep_all = keep_all * keep
            for part in range(size):
                send_s[part, :, lanes] = state[part * slab : (part + 1) * slab].astype(bf16)
            ksend_s[:, lanes] = keep_all

        def inside(turn):
            first_half = lane_iota((CHUNK, LANES)) < head_width
            for k in range(chunks):
                here = pl.ds(k * CHUNK, CHUNK)
                base = turn * group * 2
                level = pltpu.roll(l_s[here, :], heads_pad - base, 1)
                gram = gm_s[k]
                for i in range(group):
                    lanes = pl.ds(pl.multiple_of(turn * span + i * LANES, LANES), LANES)
                    mixes = []
                    for j in range(2 * i, 2 * i + 2):
                        shift = level[:, j : j + 1] - m_s[k, pl.ds(base + j, 1), :]
                        shift = jnp.minimum(shift, lg_s[k, pl.ds(base + j, 1), :])
                        mixes.append((jnp.exp2(shift) * gram).astype(bf16))
                    conv = xc_s[here, lanes]
                    zero = jnp.zeros_like(conv)
                    both = jnp.concatenate(
                        [jnp.where(first_half, conv, zero), jnp.where(first_half, zero, conv)], 0
                    )
                    out = jnp.dot(
                        jnp.concatenate(mixes, 1), both, preferred_element_type=f32
                    )
                    y_s[here, lanes] = out + keepx_s[chunks : chunks + 1, lanes] * conv.astype(f32)
            gate_copy(turn).wait()
            at = pl.ds(pl.multiple_of(turn * span, span), span)
            gate = jnp.dot(rows_s[...], wz_s[turn], preferred_element_type=f32)
            z_s[:, at] = (gate * widen(scale_ref[pl.ds(HALO, rows), :], group)).astype(bf16)

        def leave(turn):
            lanes = pl.ds(pl.multiple_of(turn * span, span), span)
            pick = selector(turn * group, 2 * heads_pad, bf16)
            keeps = keepx_s[:, lanes]
            state = jnp.concatenate(
                [inc_s[part, :, lanes].astype(f32) for part in range(size)], 0
            )
            for k in range(chunks):
                here = pl.ds(k * CHUNK, CHUNK)
                weight = jnp.dot(cw_s[here, :], pick, preferred_element_type=f32)
                carried = jnp.dot(c_s[here, :], state.astype(bf16), preferred_element_type=f32)
                out = y_s[here, lanes] + weight * carried
                gate = z_s[here, lanes].astype(f32)
                out = out * silu(gate)
                square = out * out
                sums = square[:, :LANES]
                for i in range(1, group):
                    sums += square[:, i * LANES : (i + 1) * LANES]
                ss_ref[here, :] += sums
                g_ref[here, lanes] = (out * gg_ref[0:1, lanes]).astype(bf16)
                if k < chunks - 1:
                    state = state * keeps[k : k + 1] + fresh_s[k, :, lanes]

        def send_half(half):
            for distance in range(1, size):
                target = lax.rem(me + distance, size)
                hop(send_s.at[target], recv_s.at[me], half, distance, send_sem, recv_sem).start()
                hop(ksend_s, krecv_s.at[me], half, distance, ksend_sem, krecv_sem).start()

        def scan_half(half):
            for distance in range(1, size):
                source = lax.rem(me - distance + size, size)
                hop(send_s.at[me], recv_s.at[source], half, distance, send_sem, recv_sem).wait_recv()
                hop(ksend_s, krecv_s.at[source], half, distance, ksend_sem, krecv_sem).wait_recv()
            first, end = halves[half]
            cols = slice(first * span, end * span)
            run = jnp.zeros((slab, (end - first) * span), f32)
            for part in range(size):
                back_s[part, :, cols] = run.astype(bf16)
                if part < size - 1:
                    run = run * krecv_s[part, :, cols] + recv_s[part, :, cols].astype(f32)
            for distance in range(1, size):
                target = lax.rem(me + distance, size)
                hop(back_s.at[target], inc_s.at[me], half, distance, bsend_sem, brecv_sem).start()
            inc_s[me, :, cols] = back_s[me, :, cols]

        def leave_half(half):
            for distance in range(1, size):
                source = lax.rem(me - distance + size, size)
                hop(back_s.at[me], inc_s.at[source], half, distance, bsend_sem, brecv_sem).wait_recv()
            pl.loop(*halves[half])(leave)

        pl.loop(*halves[0])(enter)
        pl.semaphore_wait(barrier, size - 1)
        send_half(0)
        pl.loop(*halves[1])(enter)
        send_half(1)
        recv_s[me] = send_s[me]
        krecv_s[me] = ksend_s[...]
        ss_ref[...] = jnp.zeros_like(ss_ref)
        rows_copy.wait()
        for i in range(3):
            if cuts[i] < cuts[i + 1]:
                pl.loop(cuts[i], cuts[i + 1])(inside)
            if i < 2:
                scan_half(i)
        for half in range(2):
            leave_half(half)

        for half in range(2):
            for distance in range(1, size):
                target = lax.rem(me + distance, size)
                hop(send_s.at[target], recv_s.at[me], half, distance, send_sem, recv_sem).wait_send()
                hop(ksend_s, krecv_s.at[me], half, distance, ksend_sem, krecv_sem).wait_send()
                hop(back_s.at[target], inc_s.at[me], half, distance, bsend_sem, brecv_sem).wait_send()


def mixer(live, x_raw, bcdt, scaled, scale, weight_zx, idc, idr, cx, bx, gg, cb, bb, hv):
    size = lax.axis_size("seq")
    rows = x_raw.shape[0] - HALO
    width = x_raw.shape[1]
    features = scaled.shape[1]
    gate_tile = 2 * LANES if width % (2 * LANES) == 0 else LANES
    keeps = -(-(rows // CHUNK + 1) // 8) * 8
    hbm = pl.BlockSpec(memory_space=pl.ANY)
    states = cb.shape[1] // 2
    heads_pad = hv.shape[1]
    chunks = rows // CHUNK
    slab = states // size
    vmem = pl.BlockSpec(memory_space=pltpu.VMEM)
    dma = pltpu.SemaphoreType.DMA((2, size - 1))
    return pl.pallas_call(
        functools.partial(mixer_kernel, live),
        out_shape=(
            jax.ShapeDtypeStruct((rows, width), bf16),
            jax.ShapeDtypeStruct((rows, LANES), f32),
        ),
        in_specs=[vmem, vmem, hbm, vmem, hbm] + [vmem] * 8,
        out_specs=(vmem, vmem),
        scratch_shapes=[
            pltpu.VMEM((3, rows, LANES), f32),
            pltpu.VMEM((rows, heads_pad), f32),
            pltpu.VMEM((chunks, heads_pad, CHUNK), f32),
            pltpu.VMEM((chunks, heads_pad, CHUNK), f32),
            pltpu.VMEM((rows, 2 * heads_pad), bf16),
            pltpu.VMEM((rows, 2 * heads_pad), bf16),
            pltpu.VMEM((keeps, heads_pad), f32),
            pltpu.VMEM((keeps, width), f32),
            pltpu.VMEM((rows, states), bf16),
            pltpu.VMEM((rows, states), bf16),
            pltpu.VMEM((chunks, CHUNK, CHUNK), f32),
            pltpu.VMEM((rows, width), bf16),
            pltpu.VMEM((chunks, states, width), f32),
            pltpu.VMEM((rows, width), f32),
            pltpu.VMEM((size, slab, width), bf16),
            pltpu.VMEM((size, slab, width), bf16),
            pltpu.VMEM((1, width), f32),
            pltpu.VMEM((size, 1, width), f32),
            pltpu.VMEM((size, slab, width), bf16),
            pltpu.VMEM((size, slab, width), bf16),
            pltpu.VMEM((rows, features), bf16),
            pltpu.VMEM((width // gate_tile, features, gate_tile), bf16),
            pltpu.VMEM((rows, width), bf16),
            pltpu.SemaphoreType.DMA,
            pltpu.SemaphoreType.DMA((width // gate_tile,)),
            dma,
            dma,
            dma,
            dma,
            dma,
            dma,
        ],
        compiler_params=pltpu.CompilerParams(
            collective_id=live, has_side_effects=True, vmem_limit_bytes=63 * 1024 * 1024
        ),
        name=f"mixer_{live}",
    )(x_raw, bcdt, scaled, scale, weight_zx, idc, idr, cx, bx, gg, cb, bb, hv)


def piece_width(features):
    return max(w for w in (512, 256, 128) if features % w == 0)


def boundary_kernel(out_live, in_live, *refs):
    refs = iter(refs)
    take = lambda count: [next(refs) for _ in range(count)]
    sends_rows = out_live is None
    if out_live is not None:
        gated_ref, squares_ref, weight_out = take(3)
    (hidden_ref,) = take(1)
    if in_live is not None:
        gain_ref, weight_zx, weight_bc, weight_dt = take(4)
    if out_live is not None:
        (done_ref,) = take(1)
    if in_live is not None:
        x_ref, small_ref, scaled_ref, scale_ref = take(4)
    if out_live is not None:
        wo_s, part_s, psend_s, precv_s, sqsend_s, sqrecv_s = take(6)
        wo_sem, psend_sem, precv_sem, sqsend_sem, sqrecv_sem = take(5)
    if in_live is not None:
        rows_s, wz_s, acc_s, accb_s, squares_s = take(5)
        wz_sem, rsend_sem, rrecv_sem, hsend_sem, hrecv_sem = take(5)

    tp = lax.axis_size("tp")
    shards = lax.axis_size("seq")
    t = lax.axis_index("tp")
    s = lax.axis_index("seq")
    pipe = lax.axis_index("pipe")
    count, features = hidden_ref.shape
    piece = piece_width(features)
    pieces = features // piece
    has_next = (t == tp - 1) & (s < shards - 1)
    from_live = in_live if sends_rows else out_live

    def peer(distance):
        return lax.rem(t + distance, tp)

    def cols(c):
        return pl.ds(c * piece, piece)

    def row_copy(source, c, distance):
        return pltpu.make_async_remote_copy(
            src_ref=source.at[:, cols(c)],
            dst_ref=rows_s.at[c, pl.ds(pl.multiple_of(HALO + t * count, HALO), count), :],
            send_sem=rsend_sem.at[c, distance],
            recv_sem=rrecv_sem.at[c, distance],
            device_id={"pipe": in_live, "tp": peer(distance)},
            device_id_type=MESH,
        )

    def row_arrival(c, distance):
        start = HALO + lax.rem(t - distance + tp, tp) * count
        return pltpu.make_async_remote_copy(
            src_ref=rows_s.at[c, pl.ds(0, count), :],
            dst_ref=rows_s.at[c, pl.ds(pl.multiple_of(start, HALO), count), :],
            send_sem=rsend_sem.at[c, distance],
            recv_sem=rrecv_sem.at[c, distance],
            device_id={"pipe": in_live, "tp": peer(distance)},
            device_id_type=MESH,
        )

    def halo_copy(source, c, target):
        return pltpu.make_async_remote_copy(
            src_ref=source.at[pl.ds(count - HALO, HALO), cols(c)],
            dst_ref=rows_s.at[c, pl.ds(0, HALO), :],
            send_sem=hsend_sem.at[c, target],
            recv_sem=hrecv_sem.at[c],
            device_id={"pipe": in_live, "seq": s + 1, "tp": target},
            device_id_type=MESH,
        )

    def part_copy(c, distance):
        return pltpu.make_async_remote_copy(
            src_ref=psend_s.at[c, peer(distance)],
            dst_ref=precv_s.at[c, distance - 1],
            send_sem=psend_sem.at[c, distance - 1],
            recv_sem=precv_sem.at[c, distance - 1],
            device_id={"tp": peer(distance)},
            device_id_type=MESH,
        )

    def square_copy(distance):
        return pltpu.make_async_remote_copy(
            src_ref=sqsend_s.at[peer(distance)],
            dst_ref=sqrecv_s.at[distance - 1],
            send_sem=sqsend_sem.at[distance - 1],
            recv_sem=sqrecv_sem.at[distance - 1],
            device_id={"tp": peer(distance)},
            device_id_type=MESH,
        )

    def greet(**where):
        pl.semaphore_signal(
            pltpu.get_barrier_semaphore(), inc=1, device_id=where, device_id_type=MESH
        )

    def meet(number, with_next):
        barrier = pltpu.get_barrier_semaphore()
        if not with_next:
            if number:
                pl.semaphore_wait(barrier, number)
            return

        @pl.when(has_next)
        def _():
            pl.semaphore_wait(barrier, number + tp)

        if number:

            @pl.when(jnp.logical_not(has_next))
            def _():
                pl.semaphore_wait(barrier, number)

    def weight_copy(c):
        return pltpu.make_async_copy(
            weight_zx.at[pl.ds(c * piece, piece), pl.ds(x_ref.shape[1], x_ref.shape[1])],
            wz_s.at[c],
            wz_sem.at[c],
        )

    def forward_rows(source, c):
        first = 1 if sends_rows else 0
        for distance in range(first, tp):
            row_copy(source, c, distance).start()

        @pl.when(has_next)
        def _():
            for target in range(tp):
                halo_copy(source, c, target).start()

    def drain_rows(source):
        for c in range(pieces):
            for distance in range(1 if sends_rows else 0, tp):
                row_copy(source, c, distance).wait_send()

        @pl.when(has_next)
        def _():
            for c in range(pieces):
                for target in range(tp):
                    halo_copy(source, c, target).wait_send()

    def project():
        for c in range(pieces):
            weight_copy(c).start()
        for distance in range(1 if sends_rows else 0, tp):
            greet(pipe=from_live, tp=lax.rem(t - distance + tp, tp))

        @pl.when(s > 0)
        def _():
            greet(pipe=from_live, seq=s - 1, tp=tp - 1)

        if sends_rows:
            meet(tp - 1, True)
            for c in range(pieces):
                forward_rows(hidden_ref, c)
            for c in range(pieces):
                mine = pl.ds(pl.multiple_of(HALO + t * count, HALO), count)
                rows_s[c, mine, :] = hidden_ref[:, cols(c)]

        @pl.when(s == 0)
        def _():
            rows_s[:, pl.ds(0, HALO), :] = jnp.zeros((pieces, HALO, piece), bf16)

        total_rows = rows_s.shape[1]
        out_cols = x_ref.shape[1]
        tile = piece_width(out_cols)
        squares_s[...] = jnp.zeros_like(squares_s)
        for c in range(pieces):
            for distance in range(1 if sends_rows else 0, tp):
                row_arrival(c, distance).wait_recv()

            @pl.when(s > 0)
            def _():
                halo_copy(hidden_ref, c, 0).wait_recv()

            weight_copy(c).wait()
            values = rows_s[c].astype(f32)
            square = values * values
            sums = square[:, :LANES]
            for i in range(1, piece // LANES):
                sums += square[:, i * LANES : (i + 1) * LANES]
            squares_s[...] += sums
            scaled_ref[:, cols(c)] = (values * gain_ref[0:1, cols(c)]).astype(bf16)
            last = c == pieces - 1
            if last:
                mean = jnp.sum(squares_s[...], axis=1, keepdims=True) / features
                scale_ref[...] = jnp.broadcast_to(
                    lax.rsqrt(mean + epsilon), (total_rows, LANES)
                )
            start = 0
            for weight in (weight_bc, weight_dt):
                at = slice(start, start + weight.shape[1])
                start += weight.shape[1]
                small = jnp.dot(
                    scaled_ref[:, cols(c)],
                    weight[pl.ds(c * piece, piece), :],
                    preferred_element_type=f32,
                )
                if c > 0:
                    small += accb_s[:, at]
                if last:
                    small_ref[:, at] = small * widen(scale_ref[...], small.shape[1] // LANES)
                else:
                    accb_s[:, at] = small

            @pl.loop(0, out_cols // tile)
            def _(n):
                at = pl.ds(pl.multiple_of(n * tile, tile), tile)
                value = jnp.dot(
                    scaled_ref[:, cols(c)], wz_s[c, :, at], preferred_element_type=f32
                )
                if c > 0:
                    value += acc_s[:, at]
                if last:
                    x_ref[:, at] = (value * widen(scale_ref[...], tile // LANES)).astype(bf16)
                else:
                    acc_s[:, at] = value

            if not sends_rows:
                mine = pl.ds(pl.multiple_of(HALO + t * count, HALO), count)
                done_ref[:, cols(c)] = rows_s[c, mine, :]
        if sends_rows:
            drain_rows(hidden_ref)

    def finish():
        for c in range(pieces):
            pltpu.make_async_copy(weight_out.at[:, cols(c)], wo_s.at[c], wo_sem.at[c]).start()
        for distance in range(1, tp):
            greet(tp=peer(distance))
        for target in range(tp):
            own = squares_ref[target * count : (target + 1) * count, :]
            sqsend_s[target] = lax.dot_general(
                jnp.ones((8, LANES), f32),
                own,
                (((1,), (1,)), ((), ())),
                precision=lax.Precision.HIGHEST,
                preferred_element_type=f32,
            )
        for c in range(pieces):
            pltpu.make_async_copy(weight_out.at[:, cols(c)], wo_s.at[c], wo_sem.at[c]).wait()
            for target in range(tp):
                value = jnp.dot(
                    gated_ref[target * count : (target + 1) * count, :],
                    wo_s[c],
                    preferred_element_type=f32,
                )
                part_s[c, target] = value
                psend_s[c, target] = value.astype(bf16)
            if c == 0:
                meet(tp - 1 if in_live is None else 2 * tp - 1, in_live is not None)
                for distance in range(1, tp):
                    square_copy(distance).start()
            for distance in range(1, tp):
                part_copy(c, distance).start()
        sums = sqsend_s[t]
        for distance in range(1, tp):
            square_copy(distance).wait_recv()
            sums += sqrecv_s[distance - 1]
        sums = lax.dot_general(
            sums,
            jnp.full((8, LANES), 0.125, f32),
            (((0,), (0,)), ((), ())),
            precision=lax.Precision.HIGHEST,
            preferred_element_type=f32,
        )
        scale = lax.rsqrt(sums / (gated_ref.shape[1] * tp) + epsilon)
        for c in range(pieces):
            total = part_s[c, t]
            for distance in range(1, tp):
                part_copy(c, distance).wait_recv()
                total += precv_s[c, distance - 1].astype(f32)
            done_ref[:, cols(c)] = (
                hidden_ref[:, cols(c)].astype(f32) + total * widen(scale, piece // LANES)
            ).astype(bf16)
            if in_live is not None:
                forward_rows(done_ref, c)
        for distance in range(1, tp):
            square_copy(distance).wait_send()
            for c in range(pieces):
                part_copy(c, distance).wait_send()
        if in_live is not None:
            drain_rows(done_ref)

    if out_live is not None:
        pl.when(pipe == out_live)(finish)
    if in_live is not None:
        pl.when(pipe == in_live)(project)
    if out_live is not None:
        idle = pipe != out_live
        if in_live is not None:
            idle = idle & (pipe != in_live)

        @pl.when(idle)
        def _():
            done_ref[...] = hidden_ref[...]


def boundary(out_live, in_live, out_args, hidden, in_args):
    tp = lax.axis_size("tp")
    count, features = hidden.shape
    piece = piece_width(features)
    pieces = features // piece
    vmem = pl.BlockSpec(memory_space=pltpu.VMEM)
    hbm = pl.BlockSpec(memory_space=pl.ANY)
    dma = pltpu.SemaphoreType.DMA
    args, specs, outs, scratch = [], [], [], []
    peers = max(1, tp - 1)
    if out_live is not None:
        args += out_args
        specs += [vmem, vmem, hbm]
    args.append(hidden)
    specs.append(vmem)
    if in_live is not None:
        args += in_args
        specs += [vmem, hbm, vmem, vmem]
    if out_live is not None:
        outs.append(jax.ShapeDtypeStruct((count, features), bf16))
        width = out_args[2].shape[0]
        scratch += [
            pltpu.VMEM((pieces, width, piece), bf16),
            pltpu.VMEM((pieces, tp, count, piece), f32),
            pltpu.VMEM((pieces, tp, count, piece), bf16),
            pltpu.VMEM((pieces, peers, count, piece), bf16),
            pltpu.VMEM((tp, 8, count), f32),
            pltpu.VMEM((peers, 8, count), f32),
            dma((pieces,)),
            dma((pieces, peers)),
            dma((pieces, peers)),
            dma((peers,)),
            dma((peers,)),
        ]
    if in_live is not None:
        rows = HALO + tp * count
        wide = in_args[1].shape[1] // 2
        small = in_args[2].shape[1] + in_args[3].shape[1]
        outs += [
            jax.ShapeDtypeStruct((rows, wide), bf16),
            jax.ShapeDtypeStruct((rows, small), f32),
            jax.ShapeDtypeStruct((rows, features), bf16),
            jax.ShapeDtypeStruct((rows, LANES), f32),
        ]
        scratch += [
            pltpu.VMEM((pieces, rows, piece), bf16),
            pltpu.VMEM((pieces, piece, wide), bf16),
            pltpu.VMEM((rows, wide), f32),
            pltpu.VMEM((rows, small), f32),
            pltpu.VMEM((rows, LANES), f32),
            dma((pieces,)),
            dma((pieces, tp)),
            dma((pieces, tp)),
            dma((pieces, tp)),
            dma((pieces,)),
        ]
    sections = lax.axis_size("pipe")
    step = 0 if out_live is None else out_live + 1
    return pl.pallas_call(
        functools.partial(boundary_kernel, out_live, in_live),
        out_shape=tuple(outs),
        in_specs=specs,
        out_specs=tuple([vmem] * len(outs)),
        scratch_shapes=scratch,
        compiler_params=pltpu.CompilerParams(
            collective_id=sections + step,
            has_side_effects=True,
            vmem_limit_bytes=63 * 1024 * 1024,
        ),
        name=f"boundary_{step}",
    )(*args)


def local(
    hidden_in,
    doc_ids,
    norm_gain,
    in_zx,
    in_bc,
    in_dt,
    conv_x,
    conv_bc,
    bias_x,
    bias_bc,
    dt_bias,
    a_log,
    d_skip,
    gated_gain,
    out_w,
):
    sections = lax.axis_size("pipe")
    local_width = gated_gain.shape[1]
    heads = dt_bias.shape[1]
    heads_pad = -(-heads // LANES) * LANES
    weight_zx = in_zx[0].reshape(in_zx.shape[1], 2 * local_width)
    weight_dt = jnp.pad(in_dt[0], ((0, 0), (0, heads_pad - heads)))
    hv = jnp.pad(
        jnp.concatenate([dt_bias, a_log, d_skip], 0), ((0, 0), (0, heads_pad - heads))
    )
    row_ids = doc_ids[0].astype(f32)
    edge = lax.ppermute(
        row_ids[-HALO:] + 1.0,
        "seq",
        [(i, i + 1) for i in range(lax.axis_size("seq") - 1)],
    )
    ids_ext = jnp.concatenate([edge - 1.0, row_ids])
    idc = jnp.broadcast_to(ids_ext[:, None], (ids_ext.shape[0], LANES))
    idr = row_ids[None, :]
    in_args = [norm_gain, weight_zx, in_bc[0], weight_dt]
    projected = boundary(None, 0, None, hidden_in[0], in_args)
    current = hidden_in[0]
    for live in range(sections):
        gated, squares = mixer(
            live,
            *projected,
            weight_zx,
            idc,
            idr,
            conv_x[0],
            bias_x,
            gated_gain,
            conv_bc[0],
            bias_bc,
            hv,
        )
        out_args = [gated, squares, out_w[0]]
        if live + 1 < sections:
            current, *projected = boundary(live, live + 1, out_args, current, in_args)
        else:
            (current,) = boundary(live, None, out_args, current, None)
    return current[None, None]


def solution(mesh):
    placed = (
        P(None, ("seq", "tp"), None),
        P(None, "seq"),
        P("pipe", None),
        P("pipe", None, None, "tp"),
        P("pipe", None, None),
        P("pipe", None, "tp"),
        P("pipe", None, "tp"),
        P("pipe", None, None),
        P("pipe", "tp"),
        P("pipe", None),
        P("pipe", "tp"),
        P("pipe", "tp"),
        P("pipe", "tp"),
        P("pipe", "tp"),
        P("pipe", "tp", None),
    )
    return jax.shard_map(
        local,
        mesh=mesh,
        in_specs=placed,
        out_specs=P("pipe", None, ("seq", "tp"), None),
        check_vma=False,
    )
```

```python
import functools

import jax
import jax.numpy as jnp
from jax import lax
from jax.experimental import pallas as pl
from jax.experimental.pallas import tpu as pltpu
from jax.sharding import PartitionSpec as P

epsilon = 1e-05
LOG2E = 1.4426950408889634
HALO = 16
CHUNK = 128
LANES = 128
MESH = pl.DeviceIdType.MESH
f32 = jnp.float32
bf16 = jnp.bfloat16


def silu(value):
    half = 0.5 * value
    return half + half * jnp.tanh(half)


def widen(value, count):
    return jnp.concatenate([value] * count, 1)


def split_pair(value):
    high = value.astype(bf16)
    low = (value - high.astype(f32)).astype(bf16)
    return jnp.concatenate([high, low], 1)


def mixer_kernel(
    live,
    x_hbm,
    bcdt_ref,
    scaled_ref,
    scale_ref,
    weight_zx,
    idc_ref,
    idr_ref,
    cx_ref,
    bx_ref,
    gg_ref,
    cb_ref,
    bb_ref,
    hv_ref,
    g_hbm,
    ss_ref,
    mask_s,
    l_s,
    m_s,
    lg_s,
    ew_s,
    cw_s,
    keep_s,
    keepx_s,
    b_s,
    c_s,
    gm_s,
    xc_s,
    fresh_s,
    y_s,
    send_s,
    recv_s,
    ksend_s,
    krecv_s,
    back_s,
    inc_s,
    rows_s,
    wz_s,
    z_s,
    x_ref,
    g_ref,
    x_sem,
    g_sem,
    rows_sem,
    wz_sem,
    send_sem,
    recv_sem,
    ksend_sem,
    krecv_sem,
    bsend_sem,
    brecv_sem,
):
    size = lax.axis_size("seq")
    me = lax.axis_index("seq")
    rows = g_ref.shape[0]
    width = g_ref.shape[1]
    chunks = rows // CHUNK
    tiles = width // LANES
    states = b_s.shape[1]
    slab = states // size
    heads_pad = hv_ref.shape[1]
    head_width = LANES // 2
    group = 2 if tiles % 2 == 0 else 1
    span = group * LANES

    def lane_iota(shape):
        return lax.broadcasted_iota(jnp.int32, shape, 1)

    def row_iota(shape):
        return lax.broadcasted_iota(jnp.int32, shape, 0)

    def selector(tile, count, dtype):
        shape = (count, span)
        hit = lax.rem(row_iota(shape), heads_pad) == tile * 2 + lane_iota(shape) // head_width
        return hit.astype(f32).astype(dtype)

    turns = tiles // group
    middle = turns // 2
    halves = [(0, middle), (middle, turns)]
    cuts = [0, turns * 3 // 10, turns * 6 // 10, turns]

    def hop(source, target_ref, half, distance, send, recv):
        first, end = halves[half]
        cols = pl.ds(first * span, (end - first) * span)
        return pltpu.make_async_remote_copy(
            src_ref=source.at[:, cols],
            dst_ref=target_ref.at[:, cols],
            send_sem=send.at[half, distance - 1],
            recv_sem=recv.at[half, distance - 1],
            device_id={"seq": lax.rem(me + distance, size)},
            device_id_type=MESH,
        )

    @pl.when(lax.axis_index("pipe") == live)
    def _():
        barrier = pltpu.get_barrier_semaphore()
        x_copy = pltpu.make_async_copy(x_hbm, x_ref, x_sem)
        x_copy.start()
        rows_copy = pltpu.make_async_copy(scaled_ref.at[pl.ds(HALO, rows)], rows_s, rows_sem)
        gate_tile = span

        def gate_copy(n):
            return pltpu.make_async_copy(
                weight_zx.at[:, pl.ds(n * gate_tile, gate_tile)], wz_s.at[n], wz_sem.at[n]
            )

        for distance in range(1, size):
            pl.semaphore_signal(
                barrier,
                inc=1,
                device_id={"seq": lax.rem(me + distance, size)},
                device_id_type=MESH,
            )

        square_shape = (CHUNK, CHUNK)
        lower = row_iota(square_shape) >= lane_iota(square_shape)
        lower_f = lower.astype(f32)
        keep_s[...] = jnp.zeros_like(keep_s)
        keep_s[chunks : chunks + 1, :] = hv_ref[2:3, :]
        rate = jnp.exp(hv_ref[1:2, :]) * -LOG2E

        @pl.loop(0, chunks)
        def _(k):
            base = pl.multiple_of(k * CHUNK, CHUNK)
            here = pl.ds(base, CHUNK)
            ids_ext = idc_ref[pl.ds(base, CHUNK + HALO), :]
            seg = ids_ext[HALO:]
            prev = ids_ext[HALO - 1 : HALO]
            last = ids_ext[HALO + CHUNK - 1 :]
            for d in range(1, 4):
                same = pltpu.roll(ids_ext, d, 0)[HALO:] == seg
                mask_s[d - 1, here, :] = same.astype(f32)
            raw = bcdt_ref[pl.ds(base + HALO, CHUNK), 2 * states :] + hv_ref[0:1, :]
            step = jnp.maximum(raw, 0.0) + jnp.log1p(jnp.exp(-jnp.abs(raw)))
            level = jnp.dot(
                lower_f,
                step * rate,
                precision=lax.Precision.HIGHEST,
                preferred_element_type=f32,
            )
            l_s[here, :] = level
            step_log = jnp.log(step) * LOG2E
            m_s[k] = (level - step_log).T
            lg_s[k] = step_log.T
            end = level[CHUNK - 1 :]
            ew_s[here, :] = split_pair(
                jnp.exp2(end - level) * step * (seg == last).astype(f32)
            )
            cw_s[here, :] = split_pair(jnp.exp2(level) * (seg == prev).astype(f32))
            keep_s[pl.ds(k, 1), :] = jnp.exp2(end) * (last == prev).astype(f32)
            for half in range(2):
                cols = pl.ds(half * states, states)
                wide = bcdt_ref[pl.ds(base, CHUNK + HALO), cols]
                total = bb_ref[0:1, cols] + cb_ref[3:4, cols] * wide[HALO:]
                for d in range(1, 4):
                    total += (
                        mask_s[d - 1, here, :]
                        * cb_ref[3 - d : 4 - d, cols]
                        * pltpu.roll(wide, d, 0)[HALO:]
                    )
                place = b_s if half == 0 else c_s
                place[here, :] = silu(total).astype(bf16)
            gram = lax.dot_general(
                c_s[here, :], b_s[here, :], (((1,), (1,)), ((), ())), preferred_element_type=f32
            )
            same_doc = seg == idr_ref[0:1, pl.ds(base, CHUNK)]
            gm_s[k] = jnp.where(lower & same_doc, gram, 0.0)

        def enter(turn):
            tile = turn * group
            lanes = pl.ds(pl.multiple_of(turn * span, span), span)
            pick = selector(tile, 2 * heads_pad, bf16)
            keeps = jnp.dot(split_pair(keep_s[...]), pick, preferred_element_type=f32)
            keepx_s[:, lanes] = keeps
            state = jnp.zeros((states, span), f32)
            keep_all = jnp.ones((1, span), f32)
            for k in range(chunks):
                here = pl.ds(k * CHUNK, CHUNK)
                wide = x_ref[pl.ds(k * CHUNK, CHUNK + HALO), lanes].astype(f32)
                total = bx_ref[0:1, lanes] + cx_ref[3:4, lanes] * wide[HALO:]
                for d in range(1, 4):
                    total += (
                        widen(mask_s[d - 1, here, :], group)
                        * cx_ref[3 - d : 4 - d, lanes]
                        * pltpu.roll(wide, d, 0)[HALO:]
                    )
                conv = silu(total)
                xc_s[here, lanes] = conv.astype(bf16)
                weight = jnp.dot(ew_s[here, :], pick, preferred_element_type=f32)
                fresh = lax.dot_general(
                    b_s[here, :],
                    (conv * weight).astype(bf16),
                    (((0,), (0,)), ((), ())),
                    preferred_element_type=f32,
                )
                fresh_s[k, :, lanes] = fresh
                keep = keeps[k : k + 1]
                state = state * keep + fresh
                keep_all = keep_all * keep
            for part in range(size):
                send_s[part, :, lanes] = state[part * slab : (part + 1) * slab].astype(bf16)
            ksend_s[:, lanes] = keep_all

        def inside(turn):
            first_half = lane_iota((CHUNK, LANES)) < head_width
            for k in range(chunks):
                here = pl.ds(k * CHUNK, CHUNK)
                base = turn * group * 2
                level = pltpu.roll(l_s[here, :], heads_pad - base, 1)
                gram = gm_s[k]
                for i in range(group):
                    lanes = pl.ds(pl.multiple_of(turn * span + i * LANES, LANES), LANES)
                    mixes = []
                    for j in range(2 * i, 2 * i + 2):
                        shift = level[:, j : j + 1] - m_s[k, pl.ds(base + j, 1), :]
                        shift = jnp.minimum(shift, lg_s[k, pl.ds(base + j, 1), :])
                        mixes.append((jnp.exp2(shift) * gram).astype(bf16))
                    conv = xc_s[here, lanes]
                    zero = jnp.zeros_like(conv)
                    both = jnp.concatenate(
                        [jnp.where(first_half, conv, zero), jnp.where(first_half, zero, conv)], 0
                    )
                    out = jnp.dot(
                        jnp.concatenate(mixes, 1), both, preferred_element_type=f32
                    )
                    y_s[here, lanes] = out + keepx_s[chunks : chunks + 1, lanes] * conv.astype(f32)
            gate_copy(turn).wait()
            at = pl.ds(pl.multiple_of(turn * span, span), span)
            gate = jnp.dot(rows_s[...], wz_s[turn], preferred_element_type=f32)
            z_s[:, at] = (gate * widen(scale_ref[pl.ds(HALO, rows), :], group)).astype(bf16)

        def leave_copy(turn):
            lanes = pl.ds(pl.multiple_of(turn * span, span), span)
            return pltpu.make_async_copy(g_ref.at[:, lanes], g_hbm.at[:, lanes], g_sem.at[turn])

        def leave(turn):
            lanes = pl.ds(pl.multiple_of(turn * span, span), span)
            pick = selector(turn * group, 2 * heads_pad, bf16)
            keeps = keepx_s[:, lanes]
            state = jnp.concatenate(
                [inc_s[part, :, lanes].astype(f32) for part in range(size)], 0
            )
            for k in range(chunks):
                here = pl.ds(k * CHUNK, CHUNK)
                weight = jnp.dot(cw_s[here, :], pick, preferred_element_type=f32)
                carried = jnp.dot(c_s[here, :], state.astype(bf16), preferred_element_type=f32)
                out = y_s[here, lanes] + weight * carried
                gate = z_s[here, lanes].astype(f32)
                out = out * silu(gate)
                square = out * out
                sums = square[:, :LANES]
                for i in range(1, group):
                    sums += square[:, i * LANES : (i + 1) * LANES]
                ss_ref[here, :] += sums
                g_ref[here, lanes] = (out * gg_ref[0:1, lanes]).astype(bf16)
                if k < chunks - 1:
                    state = state * keeps[k : k + 1] + fresh_s[k, :, lanes]
            leave_copy(turn).start()

        def send_half(half):
            for distance in range(1, size):
                target = lax.rem(me + distance, size)
                hop(send_s.at[target], recv_s.at[me], half, distance, send_sem, recv_sem).start()
                hop(ksend_s, krecv_s.at[me], half, distance, ksend_sem, krecv_sem).start()

        def scan_half(half):
            for distance in range(1, size):
                source = lax.rem(me - distance + size, size)
                hop(send_s.at[me], recv_s.at[source], half, distance, send_sem, recv_sem).wait_recv()
                hop(ksend_s, krecv_s.at[source], half, distance, ksend_sem, krecv_sem).wait_recv()
            first, end = halves[half]
            cols = slice(first * span, end * span)
            run = jnp.zeros((slab, (end - first) * span), f32)
            for part in range(size):
                back_s[part, :, cols] = run.astype(bf16)
                if part < size - 1:
                    run = run * krecv_s[part, :, cols] + recv_s[part, :, cols].astype(f32)
            for distance in range(1, size):
                target = lax.rem(me + distance, size)
                hop(back_s.at[target], inc_s.at[me], half, distance, bsend_sem, brecv_sem).start()
            inc_s[me, :, cols] = back_s[me, :, cols]

        def leave_half(half):
            for distance in range(1, size):
                source = lax.rem(me - distance + size, size)
                hop(back_s.at[me], inc_s.at[source], half, distance, bsend_sem, brecv_sem).wait_recv()
            pl.loop(*halves[half])(leave)

        x_copy.wait()
        rows_copy.start()
        for n in range(width // gate_tile):
            gate_copy(n).start()
        pl.loop(*halves[0])(enter)
        pl.semaphore_wait(barrier, size - 1)
        send_half(0)
        pl.loop(*halves[1])(enter)
        send_half(1)
        recv_s[me] = send_s[me]
        krecv_s[me] = ksend_s[...]
        ss_ref[...] = jnp.zeros_like(ss_ref)
        rows_copy.wait()
        for i in range(3):
            if cuts[i] < cuts[i + 1]:
                pl.loop(cuts[i], cuts[i + 1])(inside)
            if i < 2:
                scan_half(i)
        for half in range(2):
            leave_half(half)
        for turn in range(turns):
            leave_copy(turn).wait()

        for half in range(2):
            for distance in range(1, size):
                target = lax.rem(me + distance, size)
                hop(send_s.at[target], recv_s.at[me], half, distance, send_sem, recv_sem).wait_send()
                hop(ksend_s, krecv_s.at[me], half, distance, ksend_sem, krecv_sem).wait_send()
                hop(back_s.at[target], inc_s.at[me], half, distance, bsend_sem, brecv_sem).wait_send()


def mixer(live, x_raw, bcdt, scaled, scale, weight_zx, idc, idr, cx, bx, gg, cb, bb, hv):
    size = lax.axis_size("seq")
    rows = x_raw.shape[0] - HALO
    width = x_raw.shape[1]
    features = scaled.shape[1]
    gate_tile = 2 * LANES if width % (2 * LANES) == 0 else LANES
    keeps = -(-(rows // CHUNK + 1) // 8) * 8
    hbm = pl.BlockSpec(memory_space=pl.ANY)
    states = cb.shape[1] // 2
    heads_pad = hv.shape[1]
    chunks = rows // CHUNK
    slab = states // size
    vmem = pl.BlockSpec(memory_space=pltpu.VMEM)
    dma = pltpu.SemaphoreType.DMA((2, size - 1))
    return pl.pallas_call(
        functools.partial(mixer_kernel, live),
        out_shape=(
            jax.ShapeDtypeStruct((rows, width), bf16),
            jax.ShapeDtypeStruct((rows, LANES), f32),
        ),
        in_specs=[hbm, vmem, hbm, vmem, hbm] + [vmem] * 8,
        out_specs=(hbm, vmem),
        scratch_shapes=[
            pltpu.VMEM((3, rows, LANES), f32),
            pltpu.VMEM((rows, heads_pad), f32),
            pltpu.VMEM((chunks, heads_pad, CHUNK), f32),
            pltpu.VMEM((chunks, heads_pad, CHUNK), f32),
            pltpu.VMEM((rows, 2 * heads_pad), bf16),
            pltpu.VMEM((rows, 2 * heads_pad), bf16),
            pltpu.VMEM((keeps, heads_pad), f32),
            pltpu.VMEM((keeps, width), f32),
            pltpu.VMEM((rows, states), bf16),
            pltpu.VMEM((rows, states), bf16),
            pltpu.VMEM((chunks, CHUNK, CHUNK), f32),
            pltpu.VMEM((rows, width), bf16),
            pltpu.VMEM((chunks, states, width), f32),
            pltpu.VMEM((rows, width), f32),
            pltpu.VMEM((size, slab, width), bf16),
            pltpu.VMEM((size, slab, width), bf16),
            pltpu.VMEM((1, width), f32),
            pltpu.VMEM((size, 1, width), f32),
            pltpu.VMEM((size, slab, width), bf16),
            pltpu.VMEM((size, slab, width), bf16),
            pltpu.VMEM((rows, features), bf16),
            pltpu.VMEM((width // gate_tile, features, gate_tile), bf16),
            pltpu.VMEM((rows, width), bf16),
            pltpu.VMEM((rows + HALO, width), bf16),
            pltpu.VMEM((rows, width), bf16),
            pltpu.SemaphoreType.DMA,
            pltpu.SemaphoreType.DMA((width // gate_tile,)),
            pltpu.SemaphoreType.DMA,
            pltpu.SemaphoreType.DMA((width // gate_tile,)),
            dma,
            dma,
            dma,
            dma,
            dma,
            dma,
        ],
        compiler_params=pltpu.CompilerParams(
            collective_id=live, has_side_effects=True, vmem_limit_bytes=63 * 1024 * 1024
        ),
        name=f"mixer_{live}",
    )(x_raw, bcdt, scaled, scale, weight_zx, idc, idr, cx, bx, gg, cb, bb, hv)


def piece_width(features):
    return max(w for w in (512, 256, 128) if features % w == 0)


def boundary_kernel(out_live, in_live, *refs):
    refs = iter(refs)
    take = lambda count: [next(refs) for _ in range(count)]
    sends_rows = out_live is None
    if out_live is not None:
        gated_hbm, squares_ref, weight_out = take(3)
    (hidden_hbm,) = take(1)
    hidden_ref = hidden_hbm
    if in_live is not None:
        gain_ref, weight_zx, bc_hbm, dt_hbm = take(4)
    if out_live is not None:
        (done_ref,) = take(1)
    if in_live is not None:
        x_hbm, small_ref, scaled_hbm, scale_ref = take(4)
    if out_live is not None:
        wo_s, part_s, psend_s, precv_s, sqsend_s, sqrecv_s = take(6)
        wo_sem, psend_sem, precv_sem, sqsend_sem, sqrecv_sem = take(5)
        gated_ref, hidden_ref, gated_sem, hidden_sem = take(4)
    if in_live is not None:
        rows_s, wz_s, acc_s, accb_s, squares_s = take(5)
        wz_sem, rsend_sem, rrecv_sem, hsend_sem, hrecv_sem = take(5)
        x_ref, scaled_ref, weight_bc, weight_dt = take(4)
        x_sem, scaled_sem, small_sem = take(3)

    tp = lax.axis_size("tp")
    shards = lax.axis_size("seq")
    t = lax.axis_index("tp")
    s = lax.axis_index("seq")
    pipe = lax.axis_index("pipe")
    count, features = hidden_ref.shape
    piece = piece_width(features)
    pieces = features // piece
    has_next = (t == tp - 1) & (s < shards - 1)
    from_live = in_live if sends_rows else out_live

    def peer(distance):
        return lax.rem(t + distance, tp)

    def cols(c):
        return pl.ds(c * piece, piece)

    def row_copy(source, c, distance):
        return pltpu.make_async_remote_copy(
            src_ref=source.at[:, cols(c)],
            dst_ref=rows_s.at[c, pl.ds(pl.multiple_of(HALO + t * count, HALO), count), :],
            send_sem=rsend_sem.at[c, distance],
            recv_sem=rrecv_sem.at[c, distance],
            device_id={"pipe": in_live, "tp": peer(distance)},
            device_id_type=MESH,
        )

    def row_arrival(c, distance):
        start = HALO + lax.rem(t - distance + tp, tp) * count
        return pltpu.make_async_remote_copy(
            src_ref=rows_s.at[c, pl.ds(0, count), :],
            dst_ref=rows_s.at[c, pl.ds(pl.multiple_of(start, HALO), count), :],
            send_sem=rsend_sem.at[c, distance],
            recv_sem=rrecv_sem.at[c, distance],
            device_id={"pipe": in_live, "tp": peer(distance)},
            device_id_type=MESH,
        )

    def halo_copy(source, c, target):
        return pltpu.make_async_remote_copy(
            src_ref=source.at[pl.ds(count - HALO, HALO), cols(c)],
            dst_ref=rows_s.at[c, pl.ds(0, HALO), :],
            send_sem=hsend_sem.at[c, target],
            recv_sem=hrecv_sem.at[c],
            device_id={"pipe": in_live, "seq": s + 1, "tp": target},
            device_id_type=MESH,
        )

    def part_copy(c, distance):
        return pltpu.make_async_remote_copy(
            src_ref=psend_s.at[c, peer(distance)],
            dst_ref=precv_s.at[c, distance - 1],
            send_sem=psend_sem.at[c, distance - 1],
            recv_sem=precv_sem.at[c, distance - 1],
            device_id={"tp": peer(distance)},
            device_id_type=MESH,
        )

    def square_copy(distance):
        return pltpu.make_async_remote_copy(
            src_ref=sqsend_s.at[peer(distance)],
            dst_ref=sqrecv_s.at[distance - 1],
            send_sem=sqsend_sem.at[distance - 1],
            recv_sem=sqrecv_sem.at[distance - 1],
            device_id={"tp": peer(distance)},
            device_id_type=MESH,
        )

    def greet(**where):
        pl.semaphore_signal(
            pltpu.get_barrier_semaphore(), inc=1, device_id=where, device_id_type=MESH
        )

    def meet(number, with_next):
        barrier = pltpu.get_barrier_semaphore()
        if not with_next:
            if number:
                pl.semaphore_wait(barrier, number)
            return

        @pl.when(has_next)
        def _():
            pl.semaphore_wait(barrier, number + tp)

        if number:

            @pl.when(jnp.logical_not(has_next))
            def _():
                pl.semaphore_wait(barrier, number)

    def weight_copy(c):
        return pltpu.make_async_copy(
            weight_zx.at[pl.ds(c * piece, piece), pl.ds(x_ref.shape[1], x_ref.shape[1])],
            wz_s.at[c],
            wz_sem.at[c],
        )

    def forward_rows(source, c):
        first = 1 if sends_rows else 0
        for distance in range(first, tp):
            row_copy(source, c, distance).start()

        @pl.when(has_next)
        def _():
            for target in range(tp):
                halo_copy(source, c, target).start()

    def drain_rows(source):
        for c in range(pieces):
            for distance in range(1 if sends_rows else 0, tp):
                row_copy(source, c, distance).wait_send()

        @pl.when(has_next)
        def _():
            for c in range(pieces):
                for target in range(tp):
                    halo_copy(source, c, target).wait_send()

    def project():
        smalls = [
            pltpu.make_async_copy(bc_hbm, weight_bc, small_sem.at[0]),
            pltpu.make_async_copy(dt_hbm, weight_dt, small_sem.at[1]),
        ]
        for copy in smalls:
            copy.start()
        for c in range(pieces):
            weight_copy(c).start()

        def scaled_copy(c):
            return pltpu.make_async_copy(
                scaled_ref.at[:, cols(c)], scaled_hbm.at[:, cols(c)], scaled_sem.at[c]
            )

        for distance in range(1 if sends_rows else 0, tp):
            greet(pipe=from_live, tp=lax.rem(t - distance + tp, tp))

        @pl.when(s > 0)
        def _():
            greet(pipe=from_live, seq=s - 1, tp=tp - 1)

        if sends_rows:
            meet(tp - 1, True)
            for c in range(pieces):
                forward_rows(hidden_ref, c)
            for c in range(pieces):
                mine = pl.ds(pl.multiple_of(HALO + t * count, HALO), count)
                rows_s[c, mine, :] = hidden_ref[:, cols(c)]

        @pl.when(s == 0)
        def _():
            rows_s[:, pl.ds(0, HALO), :] = jnp.zeros((pieces, HALO, piece), bf16)

        total_rows = rows_s.shape[1]
        out_cols = x_ref.shape[1]
        tile = piece_width(out_cols)

        def x_copy(n):
            at = pl.ds(pl.multiple_of(n * tile, tile), tile)
            return pltpu.make_async_copy(x_ref.at[:, at], x_hbm.at[:, at], x_sem.at[n])

        squares_s[...] = jnp.zeros_like(squares_s)
        for c in range(pieces):
            for distance in range(1 if sends_rows else 0, tp):
                row_arrival(c, distance).wait_recv()

            @pl.when(s > 0)
            def _():
                halo_copy(hidden_ref, c, 0).wait_recv()

            weight_copy(c).wait()
            values = rows_s[c].astype(f32)
            square = values * values
            sums = square[:, :LANES]
            for i in range(1, piece // LANES):
                sums += square[:, i * LANES : (i + 1) * LANES]
            squares_s[...] += sums
            scaled_ref[:, cols(c)] = (values * gain_ref[0:1, cols(c)]).astype(bf16)
            scaled_copy(c).start()
            if c == 0:
                for copy in smalls:
                    copy.wait()
            last = c == pieces - 1
            if last:
                mean = jnp.sum(squares_s[...], axis=1, keepdims=True) / features
                scale_ref[...] = jnp.broadcast_to(
                    lax.rsqrt(mean + epsilon), (total_rows, LANES)
                )
            start = 0
            for weight in (weight_bc, weight_dt):
                at = slice(start, start + weight.shape[1])
                start += weight.shape[1]
                small = jnp.dot(
                    scaled_ref[:, cols(c)],
                    weight[pl.ds(c * piece, piece), :],
                    preferred_element_type=f32,
                )
                if c > 0:
                    small += accb_s[:, at]
                if last:
                    small_ref[:, at] = small * widen(scale_ref[...], small.shape[1] // LANES)
                else:
                    accb_s[:, at] = small

            @pl.loop(0, out_cols // tile)
            def _(n):
                at = pl.ds(pl.multiple_of(n * tile, tile), tile)
                value = jnp.dot(
                    scaled_ref[:, cols(c)], wz_s[c, :, at], preferred_element_type=f32
                )
                if c > 0:
                    value += acc_s[:, at]
                if last:
                    x_ref[:, at] = (value * widen(scale_ref[...], tile // LANES)).astype(bf16)
                    x_copy(n).start()
                else:
                    acc_s[:, at] = value

            if not sends_rows:
                mine = pl.ds(pl.multiple_of(HALO + t * count, HALO), count)
                done_ref[:, cols(c)] = rows_s[c, mine, :]
        for c in range(pieces):
            scaled_copy(c).wait()
        for n in range(out_cols // tile):
            x_copy(n).wait()
        if sends_rows:
            drain_rows(hidden_ref)

    def out_copy(c):
        return pltpu.make_async_copy(weight_out.at[:, cols(c)], wo_s.at[c], wo_sem.at[c])

    def finish():
        gated_copy = pltpu.make_async_copy(gated_hbm, gated_ref, gated_sem)
        gated_copy.start()
        for c in range(min(2, pieces)):
            out_copy(c).start()
        hidden_copy = pltpu.make_async_copy(hidden_hbm, hidden_ref, hidden_sem)
        for distance in range(1, tp):
            greet(tp=peer(distance))
        for target in range(tp):
            own = squares_ref[target * count : (target + 1) * count, :]
            sqsend_s[target] = lax.dot_general(
                jnp.ones((8, LANES), f32),
                own,
                (((1,), (1,)), ((), ())),
                precision=lax.Precision.HIGHEST,
                preferred_element_type=f32,
            )
        for c in range(pieces):
            out_copy(c).wait()
            if c + 2 < pieces:
                out_copy(c + 2).start()
            if c == 0:
                gated_copy.wait()
            if c == pieces - 1:
                hidden_copy.start()
            for target in range(tp):
                value = jnp.dot(
                    gated_ref[target * count : (target + 1) * count, :],
                    wo_s[c],
                    preferred_element_type=f32,
                )
                part_s[c, target] = value
                psend_s[c, target] = value.astype(bf16)
            if c == 0:
                meet(tp - 1 if in_live is None else 2 * tp - 1, in_live is not None)
                for distance in range(1, tp):
                    square_copy(distance).start()
            for distance in range(1, tp):
                part_copy(c, distance).start()
        sums = sqsend_s[t]
        for distance in range(1, tp):
            square_copy(distance).wait_recv()
            sums += sqrecv_s[distance - 1]
        sums = lax.dot_general(
            sums,
            jnp.full((8, LANES), 0.125, f32),
            (((0,), (0,)), ((), ())),
            precision=lax.Precision.HIGHEST,
            preferred_element_type=f32,
        )
        hidden_copy.wait()
        scale = lax.rsqrt(sums / (gated_ref.shape[1] * tp) + epsilon)
        for c in range(pieces):
            total = part_s[c, t]
            for distance in range(1, tp):
                part_copy(c, distance).wait_recv()
                total += precv_s[c, distance - 1].astype(f32)
            done_ref[:, cols(c)] = (
                hidden_ref[:, cols(c)].astype(f32) + total * widen(scale, piece // LANES)
            ).astype(bf16)
            if in_live is not None:
                forward_rows(done_ref, c)
        for distance in range(1, tp):
            square_copy(distance).wait_send()
            for c in range(pieces):
                part_copy(c, distance).wait_send()
        if in_live is not None:
            drain_rows(done_ref)

    if out_live is not None:
        pl.when(pipe == out_live)(finish)
    if in_live is not None:
        pl.when(pipe == in_live)(project)
    if out_live is not None:
        idle = pipe != out_live
        if in_live is not None:
            idle = idle & (pipe != in_live)

        @pl.when(idle)
        def _():
            hidden_copy = pltpu.make_async_copy(hidden_hbm, hidden_ref, hidden_sem)
            hidden_copy.start()
            hidden_copy.wait()
            done_ref[...] = hidden_ref[...]


def boundary(out_live, in_live, out_args, hidden, in_args):
    tp = lax.axis_size("tp")
    count, features = hidden.shape
    piece = piece_width(features)
    pieces = features // piece
    vmem = pl.BlockSpec(memory_space=pltpu.VMEM)
    hbm = pl.BlockSpec(memory_space=pl.ANY)
    dma = pltpu.SemaphoreType.DMA
    args, specs, outs, scratch, out_specs = [], [], [], [], []
    peers = max(1, tp - 1)
    if out_live is not None:
        args += out_args
        specs += [hbm, vmem, hbm]
    args.append(hidden)
    specs.append(vmem if out_live is None else hbm)
    if in_live is not None:
        args += in_args
        specs += [vmem, hbm, hbm, hbm]
    if out_live is not None:
        outs.append(jax.ShapeDtypeStruct((count, features), bf16))
        out_specs.append(vmem)
        width = out_args[2].shape[0]
        scratch += [
            pltpu.VMEM((pieces, width, piece), bf16),
            pltpu.VMEM((pieces, tp, count, piece), f32),
            pltpu.VMEM((pieces, tp, count, piece), bf16),
            pltpu.VMEM((pieces, peers, count, piece), bf16),
            pltpu.VMEM((tp, 8, count), f32),
            pltpu.VMEM((peers, 8, count), f32),
            dma((pieces,)),
            dma((pieces, peers)),
            dma((pieces, peers)),
            dma((peers,)),
            dma((peers,)),
            pltpu.VMEM((tp * count, width), bf16),
            pltpu.VMEM((count, features), bf16),
            dma,
            dma,
        ]
    if in_live is not None:
        rows = HALO + tp * count
        wide = in_args[1].shape[1] // 2
        small = in_args[2].shape[1] + in_args[3].shape[1]
        out_specs += [hbm, vmem, hbm, vmem]
        outs += [
            jax.ShapeDtypeStruct((rows, wide), bf16),
            jax.ShapeDtypeStruct((rows, small), f32),
            jax.ShapeDtypeStruct((rows, features), bf16),
            jax.ShapeDtypeStruct((rows, LANES), f32),
        ]
        scratch += [
            pltpu.VMEM((pieces, rows, piece), bf16),
            pltpu.VMEM((pieces, piece, wide), bf16),
            pltpu.VMEM((rows, wide), f32),
            pltpu.VMEM((rows, small), f32),
            pltpu.VMEM((rows, LANES), f32),
            dma((pieces,)),
            dma((pieces, tp)),
            dma((pieces, tp)),
            dma((pieces, tp)),
            dma((pieces,)),
            pltpu.VMEM((rows, wide), bf16),
            pltpu.VMEM((rows, features), bf16),
            pltpu.VMEM(in_args[2].shape, bf16),
            pltpu.VMEM(in_args[3].shape, bf16),
            dma((wide // piece_width(wide),)),
            dma((pieces,)),
            dma((2,)),
        ]
    sections = lax.axis_size("pipe")
    step = 0 if out_live is None else out_live + 1
    return pl.pallas_call(
        functools.partial(boundary_kernel, out_live, in_live),
        out_shape=tuple(outs),
        in_specs=specs,
        out_specs=tuple(out_specs),
        scratch_shapes=scratch,
        compiler_params=pltpu.CompilerParams(
            collective_id=sections + step,
            has_side_effects=True,
            vmem_limit_bytes=63 * 1024 * 1024,
        ),
        name=f"boundary_{step}",
    )(*args)


def local(
    hidden_in,
    doc_ids,
    norm_gain,
    in_zx,
    in_bc,
    in_dt,
    conv_x,
    conv_bc,
    bias_x,
    bias_bc,
    dt_bias,
    a_log,
    d_skip,
    gated_gain,
    out_w,
):
    sections = lax.axis_size("pipe")
    local_width = gated_gain.shape[1]
    heads = dt_bias.shape[1]
    heads_pad = -(-heads // LANES) * LANES
    weight_zx = in_zx[0].reshape(in_zx.shape[1], 2 * local_width)
    weight_dt = jnp.pad(in_dt[0], ((0, 0), (0, heads_pad - heads)))
    hv = jnp.pad(
        jnp.concatenate([dt_bias, a_log, d_skip], 0), ((0, 0), (0, heads_pad - heads))
    )
    row_ids = doc_ids[0].astype(f32)
    edge = lax.ppermute(
        row_ids[-HALO:] + 1.0,
        "seq",
        [(i, i + 1) for i in range(lax.axis_size("seq") - 1)],
    )
    ids_ext = jnp.concatenate([edge - 1.0, row_ids])
    idc = jnp.broadcast_to(ids_ext[:, None], (ids_ext.shape[0], LANES))
    idr = row_ids[None, :]
    in_args = [norm_gain, weight_zx, in_bc[0], weight_dt]
    projected = boundary(None, 0, None, hidden_in[0], in_args)
    current = hidden_in[0]
    for live in range(sections):
        gated, squares = mixer(
            live,
            *projected,
            weight_zx,
            idc,
            idr,
            conv_x[0],
            bias_x,
            gated_gain,
            conv_bc[0],
            bias_bc,
            hv,
        )
        out_args = [gated, squares, out_w[0]]
        if live + 1 < sections:
            current, *projected = boundary(live, live + 1, out_args, current, in_args)
        else:
            (current,) = boundary(live, None, out_args, current, None)
    return current[None, None]


def solution(mesh):
    placed = (
        P(None, ("seq", "tp"), None),
        P(None, "seq"),
        P("pipe", None),
        P("pipe", None, None, "tp"),
        P("pipe", None, None),
        P("pipe", None, "tp"),
        P("pipe", None, "tp"),
        P("pipe", None, None),
        P("pipe", "tp"),
        P("pipe", None),
        P("pipe", "tp"),
        P("pipe", "tp"),
        P("pipe", "tp"),
        P("pipe", "tp"),
        P("pipe", "tp", None),
    )
    return jax.shard_map(
        local,
        mesh=mesh,
        in_specs=placed,
        out_specs=P("pipe", None, ("seq", "tp"), None),
        check_vma=False,
    )
```
